32 devices in a mesh: node: 4 (over y, x), space: 8 (over z, core).
Axes of the slice: x: 2, y: 2, z: 4, core: 2. Of those that a mesh axis runs over, the one named last changes fastest.
Arguments:
- initial: float32 [2, 512, 4096], P(None, 'space'), may hold values from 0 to 1
- sections: float32 [4, 2, 512, 4096], P('node', None, 'space'), may hold values from 0 to 1
- feed_rate: float32 [512, 4096], P('space'), may hold values from 0.02 to 0.12
- kill_rate: float32 [512, 4096], P('space'), may hold values from 0.04 to 0.12
Outputs:
- new_sections: float32 [4, 2, 512, 4096], P('node', None, 'space')
- residual_max: float32 [], replicated
The draws below stay inside these ranges and needn't reach their ends.
All inputs are finite; a program needn't handle non-finite values.
Results may differ from the reference program's by a relative error of at most 0.000094.
Values sent between devices are 32-bit elements; how exact they have to be, the bound alone decides.
A program may use at most 64 MiB of HBM per device.

```python
import math
import jax
import jax.numpy as jnp
import numpy as np
from jax import lax

NY = 4096
SWEEPS = 6
M = 4
NX = 512


def steps_of(key, extent, cuts, low, high):
    def one(position, shards_of):
        draws = jax.random.uniform(jax.random.fold_in(jax.random.fold_in(key, 6), position), (shards_of,), jnp.float32, low / len(cuts), high / len(cuts))
        return jnp.repeat(jnp.exp(draws), extent[position] // shards_of).reshape((-1,) + (1,) * (len(extent) - position - 1))

    level = one(*cuts[0])
    for cut in cuts[1:]:
        level = level * one(*cut)
    return level


def setup_inputs(seed: int = 0) -> dict:
    arg_keys = jax.random.split(jax.random.key(seed), 5)
    return {
        "initial": jnp.clip(1.0 * jax.random.uniform(arg_keys[0], (2, NX, NY), jnp.float32) ** steps_of(arg_keys[0], (2, NX, NY), ((1, 8),), -0.2, 0.2), 0.0, 1.0),
        "sections": jnp.clip(1.0 * jax.random.uniform(arg_keys[1], (M, 2, NX, NY), jnp.float32) ** steps_of(arg_keys[1], (M, 2, NX, NY), ((0, 4), (2, 8)), -0.2, 0.2), 0.0, 1.0),
        "feed_rate": jnp.clip(jnp.exp(math.log(0.12) - 1.7917595 * jax.random.uniform(arg_keys[2], (NX, NY), jnp.float32) ** steps_of(arg_keys[2], (NX, NY), ((0, 8),), -0.2, 0.2)), 0.02, 0.12),
        "kill_rate": jnp.clip(jnp.exp(math.log(0.12) - 1.0986123 * jax.random.uniform(arg_keys[3], (NX, NY), jnp.float32) ** steps_of(arg_keys[3], (NX, NY), ((0, 8),), -0.2, 0.2)), 0.04, 0.12),
    }


step_size = 4.0
diff_u = 1.0
diff_v = 0.5


def radau_target(order, value):
    before = 1.0
    current = value
    previous = 1.0
    for degree in range(1, order):
        following = ((2 * degree + 1) * value * current - degree * before) / (degree + 1)
        before = current
        current = following
    if order == 1:
        previous = 1.0
    else:
        previous = before
    return current - previous


def radau_table(total):
    grid_count = 20000
    roots_found = []
    left_value = -1.0
    left_target = radau_target(total, left_value)
    for step_index in range(1, grid_count):
        right_value = -1.0 + 2.0 * step_index / grid_count
        right_target = radau_target(total, right_value)
        if left_target * right_target < 0.0:
            lower = left_value
            upper = right_value
            lower_target = left_target
            for bisect_index in range(80):
                halfway = 0.5 * (lower + upper)
                halfway_target = radau_target(total, halfway)
                if lower_target * halfway_target <= 0.0:
                    upper = halfway
                else:
                    lower = halfway
                    lower_target = halfway_target
            roots_found.append(0.5 * (lower + upper))
        left_value = right_value
        left_target = right_target
    roots_found.append(1.0)
    points = [(value + 1.0) / 2.0 for value in roots_found]
    quad_rows = []
    for node_index in range(total):
        row_values = []
        for basis_index in range(total):
            coefs = [1.0]
            for other_index in range(total):
                if other_index != basis_index:
                    scale = 1.0 / (points[basis_index] - points[other_index])
                    shifted = [0.0] + coefs
                    widened = coefs + [0.0]
                    coefs = [(shifted[k] - points[other_index] * widened[k]) * scale for k in range(len(shifted))]
            integral = 0.0
            for power_index in range(len(coefs)):
                integral += coefs[power_index] * points[node_index] ** (power_index + 1) / (power_index + 1)
            row_values.append(integral)
        quad_rows.append(row_values)
    return np.array(points), np.array(quad_rows)


def neighbours(field):
    return (jnp.roll(field, -1, 2) + jnp.roll(field, 1, 2)) + (jnp.roll(field, -1, 3) + jnp.roll(field, 1, 3))


def reference(initial, sections, feed_rate, kill_rate):
    points, quad_matrix = radau_table(M)
    points = jnp.asarray(points, jnp.float32)
    quad_matrix = jnp.asarray(quad_matrix, jnp.float32)
    diffusivity = jnp.array([diff_u, diff_v], jnp.float32).reshape(1, 2, 1, 1)
    laplace = neighbours(sections) - 4.0 * sections
    implicit = diffusivity * laplace
    species_u = sections[:, 0]
    species_v = sections[:, 1]
    product = species_u * species_v * species_v
    reaction = jnp.stack((-product + feed_rate * (1.0 - species_u), product - (feed_rate + kill_rate) * species_v), axis=1)
    slopes = implicit + reaction
    summed = jnp.einsum("mj,jsxy->msxy", quad_matrix, slopes, precision=lax.Precision.HIGHEST)
    quadrature = initial[None] + step_size * summed
    residual_max = jnp.max(jnp.abs(quadrature - sections))
    node_step = (step_size * points).reshape(M, 1, 1, 1)
    right_side = quadrature - node_step * implicit
    coupling = node_step * diffusivity
    divisor = 4.0 * coupling + 1.0
    iterate = sections
    for sweep_index in range(SWEEPS):
        iterate = (right_side + coupling * neighbours(iterate)) / divisor
    return iterate, residual_max
```

```python
import functools

import jax
import jax.numpy as jnp
import numpy as np
from jax import lax
from jax.experimental import pallas as pl
from jax.experimental.pallas import tpu as pltpu
from jax.sharding import PartitionSpec as P

SWEEPS = 6


step_size = 4.0
diff_u = 1.0
diff_v = 0.5


def radau_target(order, value):
    before = 1.0
    current = value
    previous = 1.0
    for degree in range(1, order):
        following = ((2 * degree + 1) * value * current - degree * before) / (degree + 1)
        before = current
        current = following
    previous = before
    return current - previous


def radau_table(total):
    grid_count = 20000
    roots_found = []
    left_value = -1.0
    left_target = radau_target(total, left_value)
    for step_index in range(1, grid_count):
        right_value = -1.0 + 2.0 * step_index / grid_count
        right_target = radau_target(total, right_value)
        if left_target * right_target < 0.0:
            lower = left_value
            upper = right_value
            lower_target = left_target
            for bisect_index in range(80):
                halfway = 0.5 * (lower + upper)
                halfway_target = radau_target(total, halfway)
                if lower_target * halfway_target <= 0.0:
                    upper = halfway
                else:
                    lower = halfway
                    lower_target = halfway_target
            roots_found.append(0.5 * (lower + upper))
        left_value = right_value
        left_target = right_target
    roots_found.append(1.0)
    points = [(value + 1.0) / 2.0 for value in roots_found]
    quad_rows = []
    for node_index in range(total):
        row_values = []
        for basis_index in range(total):
            coefs = [1.0]
            for other_index in range(total):
                if other_index != basis_index:
                    scale = 1.0 / (points[basis_index] - points[other_index])
                    shifted = [0.0] + coefs
                    widened = coefs + [0.0]
                    coefs = [
                        (shifted[k] - points[other_index] * widened[k]) * scale
                        for k in range(len(shifted))
                    ]
            integral = 0.0
            for power_index in range(len(coefs)):
                integral += (
                    coefs[power_index] * points[node_index] ** (power_index + 1) / (power_index + 1)
                )
            row_values.append(integral)
        quad_rows.append(row_values)
    return (np.array(points), np.array(quad_rows))


MESH = pl.DeviceIdType.MESH
LANES = 128
EDGE = 8
TOP = 2 * EDGE


def kernel(
    nodes,
    spaces,
    table,
    sections,
    feed_rate,
    kill_rate,
    initial,
    out,
    residual,
    sec,
    feed,
    kill,
    init,
    other,
    pack_out,
    pack_in,
    mixed,
    side,
    works_a,
    works_b,
    works_c,
    works_d,
    works_e,
    peak,
    peaks_node,
    peaks_space,
    local_sem,
    halo_sem,
    other_sem,
    pack_sem,
    first_sem,
    second_sem,
    side_sem,
    peak_node_sem,
    peak_space_sem,
):
    works = (works_a, works_b, works_c, works_d, works_e)
    cols = sec.shape[1]
    rows = feed.shape[1]
    block = cols // nodes
    me = lax.axis_index("node")
    here = lax.axis_index("space")
    tall = 2 if nodes % 2 == 0 else 1
    wide = nodes // tall
    chunks = (
        (0, TOP),
        (rows - TOP, TOP),
        (TOP, rows - 5 * EDGE),
        (rows - 3 * EDGE, EDGE),
    )
    pieces = (
        (0, EDGE),
        (rows - EDGE, EDGE),
        (EDGE, rows - 5 * EDGE),
        (rows - 4 * EDGE, 2 * EDGE),
        (rows - 2 * EDGE, EDGE),
    )
    own = me * block

    def ahead(o):
        return ((me // wide + o // wide) % tall) * wide + (me % wide + o % wide) % wide

    def negated(o):
        return ((tall - o // wide) % tall) * wide + (wide - o % wide) % wide

    def fetch(source, target, start, size, offset, sem):
        for k in range(start // EDGE, (start + size) // EDGE):
            pltpu.make_async_copy(
                source.at[k], target.at[:, pl.ds(offset + k * EDGE, EDGE)], sem
            ).start()

    def arrived_in(ref, sem):
        pltpu.make_async_copy(ref, ref, sem).wait()

    for i, (start, size) in enumerate(chunks):
        for s in range(2):
            fetch(sections.at[s], sec.at[s], start, size, TOP, local_sem.at[i])

    barrier = pltpu.get_barrier_semaphore()
    for o in range(1, nodes):
        pl.semaphore_signal(barrier, inc=1, device_id={"node": ahead(o)}, device_id_type=MESH)
    for o in range(1, spaces):
        pl.semaphore_signal(
            barrier, inc=1, device_id={"space": (here + o) % spaces}, device_id_type=MESH
        )

    mine = pl.ds(own, block)
    fetch(feed_rate.at[:, mine], feed, 0, rows, 0, local_sem.at[4])
    fetch(kill_rate.at[:, mine], kill, 0, rows, 0, local_sem.at[5])
    for s in range(2):
        fetch(initial.at[s, :, mine], init.at[s], 0, rows, 0, local_sem.at[6])

    def along(ref, sem, way):
        start = TOP + rows - EDGE if way == 0 else TOP
        land = TOP - EDGE if way == 0 else TOP + rows
        target = (here + 1) % spaces if way == 0 else (here + spaces - 1) % spaces
        return pltpu.make_async_remote_copy(
            src_ref=ref.at[:, pl.ds(start, EDGE)],
            dst_ref=ref.at[:, pl.ds(land, EDGE)],
            send_sem=sem.at[0, way],
            recv_sem=sem.at[1, way],
            device_id={"space": target},
            device_id_type=MESH,
        )

    def halo(ref, sem, s, way):
        return along(ref.at[s], sem.at[s], way)

    def forward(o, s, way):
        return along(other.at[o - 1, s, pl.ds(1, block)], other_sem.at[o - 1, s], way)

    def first(p, o):
        start, size = chunks[p]
        where = pl.ds(TOP + start, size)
        return pltpu.make_async_remote_copy(
            src_ref=sec.at[:, pl.ds(ahead(o) * block, block), where],
            dst_ref=other.at[o - 1, :, pl.ds(1, block), where],
            send_sem=first_sem.at[0, p, o - 1],
            recv_sem=first_sem.at[1, p, o - 1],
            device_id={"node": ahead(o)},
            device_id_type=MESH,
        )

    def packed(o):
        return pltpu.make_async_remote_copy(
            src_ref=pack_out.at[o - 1],
            dst_ref=pack_in.at[o - 1],
            send_sem=pack_sem.at[0, o - 1],
            recv_sem=pack_sem.at[1, o - 1],
            device_id={"node": ahead(o)},
            device_id_type=MESH,
        )

    def second(s, p, o):
        start, size = pieces[p]
        return pltpu.make_async_remote_copy(
            src_ref=mixed.at[o - 1, s, :, pl.ds(start, size)],
            dst_ref=side.at[s, mine, pl.ds(TOP + start, size)],
            send_sem=second_sem.at[0, s, p, o - 1],
            recv_sem=second_sem.at[1, s, p, o - 1],
            device_id={"node": ahead(o)},
            device_id_type=MESH,
        )

    order = tuple(range(nodes - 1, 0, -1))
    lane = lax.broadcasted_iota(jnp.int32, (EDGE, LANES), 1)

    def chunk_arrived(i):
        start, size = chunks[i]
        arrived_in(sec.at[:, :, pl.ds(TOP + start, size)], local_sem.at[i])

    chunk_arrived(0)
    chunk_arrived(1)
    pl.semaphore_wait(barrier, nodes - 1 + spaces - 1)
    for p in range(2):
        for o in order:
            first(p, o).start()
    for s in range(2):
        for way in range(2):
            halo(sec, halo_sem, s, way).start()
    chunk_arrived(2)
    chunk_arrived(3)

    groups = rows // EDGE
    for o in order:
        left = (ahead(o) * block + cols - 1) % cols
        right = (ahead(o) * block + block) % cols
        for s in range(2):
            pack = jnp.zeros((EDGE, LANES), jnp.float32)
            for g in range(groups):
                at = pl.ds(TOP + g * EDGE, EDGE)
                both = jnp.where(lane == LANES - 1, sec[s, left, at, :], sec[s, right, at, :])
                pack = jnp.where(lane // 2 == g, pltpu.roll(both, 2 * g + 1, 1), pack)
            pack_out[o - 1, s] = pack
        packed(o).start()
    for p in range(2, 4):
        for o in order:
            first(p, o).start()

    arrived_in(feed, local_sem.at[4])
    arrived_in(kill, local_sem.at[5])
    arrived_in(init, local_sem.at[6])

    for o in order:
        for p in range(2):
            first(p, o).wait_recv()
        for s in range(2):
            for way in range(2):
                forward(o, s, way).start()
    for o in order:
        packed(o).wait_recv()
        for s in range(2):
            pack = pack_in[o - 1, s]
            for g in range(groups):
                at = pl.ds(TOP + g * EDGE, EDGE)
                both = pltpu.roll(pack, LANES - 1 - 2 * g, 1)
                other[o - 1, s, 0, at, :] = both
                other[o - 1, s, block + 1, at, :] = both
    for s in range(2):
        for way in range(2):
            halo(sec, halo_sem, s, way).wait_recv()
    for o in order:
        for s in range(2):
            for way in range(2):
                forward(o, s, way).wait_recv()

    diffs = (diff_u, diff_v)
    sources = [me] + [ahead(negated(o)) for o in range(1, nodes)]
    targets = [me] + [ahead(o) for o in range(1, nodes)]
    weights = [[table[m * nodes + j] for j in sources] for m in targets]
    steps = [table[nodes * nodes + m] for m in targets]
    inverses = [
        [table[nodes * nodes + (1 + s) * nodes + m] for m in targets] for s in range(2)
    ]

    def ringed(left, middle, right, start):
        at = pl.ds(TOP + start, EDGE)
        here_tile = middle[at, :]
        before = pltpu.roll(jnp.where(lane == LANES - 1, left[at, :], here_tile), 1, 1)
        after = pltpu.roll(jnp.where(lane == 0, right[at, :], here_tile), LANES - 1, 1)
        below = middle[pl.ds(TOP + start + 1, EDGE), :]
        above = middle[pl.ds(TOP + start - 1, EDGE), :]
        return here_tile, (below + above) + (after + before)

    def mix(starts, worst):
        def one(c, worst):
            here_column = own + c
            left = (own + c + cols - 1) % cols
            right = (own + c + 1) % cols
            for start in starts:
                at = pl.ds(start, EDGE)
                f = feed[c, at, :]
                both_rates = f + kill[c, at, :]
                fields, laps, slopes = ([], []), ([], []), ([], [])
                for slot in range(nodes):
                    for s in range(2):
                        if slot == 0:
                            tiles = [sec.at[s, k] for k in (left, here_column, right)]
                        else:
                            tiles = [other.at[slot - 1, s, c + k] for k in range(3)]
                        w, ring = ringed(*tiles, start)
                        fields[s].append(w)
                        laps[s].append(diffs[s] * (ring - 4.0 * w))
                    u, v = fields[0][slot], fields[1][slot]
                    product = u * v * v
                    slopes[0].append(laps[0][slot] + (f * (1.0 - u) - product))
                    slopes[1].append(laps[1][slot] + (product - both_rates * v))
                for s in range(2):
                    base = init[s, c, at, :]
                    for t in range(nodes):
                        to = negated(t)
                        total = weights[t][0] * slopes[s][0]
                        for j in range(1, nodes):
                            total = total + weights[t][j] * slopes[s][j]
                        total = base + total
                        worst = jnp.maximum(worst, jnp.abs(total - fields[s][to]))
                        value = (total - steps[t] * laps[s][to]) * inverses[s][t]
                        if t == 0:
                            side[s, here_column, pl.ds(TOP + start, EDGE), :] = value
                        else:
                            mixed[t - 1, s, c, at, :] = value
            return worst

        return lax.fori_loop(0, block, one, worst)

    def send_back(s, ps):
        for p in ps:
            for o in order:
                second(s, p, o).start()

    def starts_of(ps):
        return [low for p in ps for low in range(pieces[p][0], sum(pieces[p]), EDGE)]

    worst = jnp.zeros((EDGE, LANES), jnp.float32)
    worst = mix(starts_of((0, 1)), worst)
    send_back(0, (0, 1))
    for o in order:
        first(2, o).wait_recv()
    worst = mix(starts_of((2,)), worst)
    send_back(0, (2,))
    for o in order:
        first(3, o).wait_recv()
    worst = mix(starts_of((3, 4)), worst)
    peak[0] = worst

    def peak_node(o):
        return pltpu.make_async_remote_copy(
            src_ref=peak.at[0],
            dst_ref=peaks_node.at[o - 1],
            send_sem=peak_node_sem.at[0, o - 1],
            recv_sem=peak_node_sem.at[1, o - 1],
            device_id={"node": ahead(o)},
            device_id_type=MESH,
        )

    def peak_space(o):
        return pltpu.make_async_remote_copy(
            src_ref=peak.at[1],
            dst_ref=peaks_space.at[o - 1],
            send_sem=peak_space_sem.at[0, o - 1],
            recv_sem=peak_space_sem.at[1, o - 1],
            device_id={"space": (here + o) % spaces},
            device_id_type=MESH,
        )

    for o in range(1, nodes):
        peak_node(o).start()
    send_back(0, (3, 4))
    send_back(1, range(len(pieces)))

    inverse = [inverses[s][0] for s in range(2)]
    factor = [steps[0] * diffs[s] * inverse[s] for s in range(2)]

    def around(ref, s, start, size):
        narrow = lax.broadcasted_iota(jnp.int32, (size, LANES), 1)
        at = pl.ds(start, size)
        tiles = [ref[s, k, at, :] for k in range(cols)]
        sums = []
        for k in range(cols):
            before, tile, after = tiles[k - 1], tiles[k], tiles[(k + 1) % cols]
            left = pltpu.roll(jnp.where(narrow == LANES - 1, before, tile), 1, 1)
            right = pltpu.roll(jnp.where(narrow == 0, after, tile), LANES - 1, 1)
            below = ref[s, k, pl.ds(start + 1, size), :]
            above = ref[s, k, pl.ds(start - 1, size), :]
            sums.append((below + above) + (right + left))
        return sums

    def band(s, spans):
        for k, (start, stop) in enumerate(spans):
            source, plane = (sec, s) if k == 0 else (works[k - 1], 0)
            for low in range(TOP + start, TOP + stop, EDGE):
                size = min(EDGE, TOP + stop - low)
                sums = around(source, plane, low, size)
                for c in range(cols):
                    value = side[s, c, pl.ds(low, size), :] + factor[s] * sums[c]
                    if k == SWEEPS - 1:
                        out[s, (low - TOP) // EDGE, c] = value
                    else:
                        works[k][0, c, pl.ds(low, size), :] = value

    reach = SWEEPS - 1
    cut = rows - 4 * EDGE
    late = rows - 2 * EDGE
    lower = [(k - reach, cut + reach - k - EDGE) for k in range(SWEEPS)]
    middle = [(cut + reach - k - EDGE, late - k) for k in range(reach)] + [(cut - EDGE, cut + EDGE)]
    upper = [(late + EDGE + k, rows + reach - k) for k in range(reach)]
    last = [(late - k, late + EDGE + k) for k in range(reach)] + [(cut + EDGE, rows)]

    def returned(s, p):
        for o in order:
            second(s, p, o).wait_recv()

    for s in range(2):
        returned(s, 0)
        returned(s, 1)
        for way in range(2):
            halo(side, side_sem, s, way).start()
        if s == 0:
            for o in range(1, nodes):
                peak_node(o).wait_recv()
            peak[1] = jnp.maximum(peak[0], jnp.max(peaks_node[...], axis=0))
            for o in range(1, spaces):
                peak_space(o).start()
        returned(s, 2)
        for way in range(2):
            halo(side, side_sem, s, way).wait_recv()
        band(s, lower)
        returned(s, 3)
        band(s, upper)
        band(s, middle)
        if s == 1:
            for o in range(1, spaces):
                peak_space(o).wait_recv()
            residual[0, 0] = jnp.max(jnp.maximum(peak[1], jnp.max(peaks_space[...], axis=0)))
        returned(s, 4)
        band(s, last)

    for o in order:
        packed(o).wait_send()
        for p in range(len(chunks)):
            first(p, o).wait_send()
    for s in range(2):
        for way in range(2):
            halo(sec, halo_sem, s, way).wait_send()
            halo(side, side_sem, s, way).wait_send()
            for o in order:
                forward(o, s, way).wait_send()
        for p in range(len(pieces)):
            for o in order:
                second(s, p, o).wait_send()
    for o in range(1, nodes):
        peak_node(o).wait_send()
    for o in range(1, spaces):
        peak_space(o).wait_send()


def shards(initial, sections, feed_rate, kill_rate):
    nodes = lax.axis_size("node")
    spaces = lax.axis_size("space")
    rows, columns = feed_rate.shape
    cols = columns // LANES
    block = cols // nodes
    points, quad_matrix = radau_table(nodes)
    steps = step_size * np.float32(points)
    table = np.concatenate(
        [
            step_size * np.float32(quad_matrix).reshape(-1),
            steps,
            1.0 / (4.0 * (steps * diff_u) + 1.0),
            1.0 / (4.0 * (steps * diff_v) + 1.0),
        ]
    ).astype(np.float32)
    high = TOP + rows + TOP
    f32 = jnp.float32

    def tiled(array):
        split = array.reshape(*array.shape[:-2], rows // EDGE, EDGE, cols, LANES)
        return jnp.swapaxes(split, -3, -2)

    any_spec = pl.BlockSpec(memory_space=pl.ANY)
    dma = pltpu.SemaphoreType.DMA
    result, residual = pl.pallas_call(
        functools.partial(kernel, nodes, spaces),
        out_shape=(
            pltpu.VMEM((2, rows // EDGE, cols, EDGE, LANES), f32),
            jax.ShapeDtypeStruct((1, 1), f32),
        ),
        in_specs=[pl.BlockSpec(memory_space=pltpu.SMEM)] + [any_spec] * 4,
        out_specs=(pl.BlockSpec(memory_space=pltpu.VMEM), pl.BlockSpec(memory_space=pltpu.SMEM)),
        scratch_shapes=[
            pltpu.VMEM((2, cols, high, LANES), f32),
            pltpu.VMEM((block, rows, LANES), f32),
            pltpu.VMEM((block, rows, LANES), f32),
            pltpu.VMEM((2, block, rows, LANES), f32),
            pltpu.VMEM((nodes - 1, 2, block + 2, high, LANES), f32),
            pltpu.VMEM((nodes - 1, 2, EDGE, LANES), f32),
            pltpu.VMEM((nodes - 1, 2, EDGE, LANES), f32),
            pltpu.VMEM((nodes - 1, 2, block, rows, LANES), f32),
            pltpu.VMEM((2, cols, high, LANES), f32),
            *[pltpu.VMEM((1, cols, high, LANES), f32)] * (SWEEPS - 1),
            pltpu.VMEM((2, EDGE, LANES), f32),
            pltpu.VMEM((nodes - 1, EDGE, LANES), f32),
            pltpu.VMEM((spaces - 1, EDGE, LANES), f32),
            dma((7,)),
            dma((2, 2, 2)),
            dma((nodes - 1, 2, 2, 2)),
            dma((2, nodes - 1)),
            dma((2, 4, nodes - 1)),
            dma((2, 2, 5, nodes - 1)),
            dma((2, 2, 2)),
            dma((2, nodes - 1)),
            dma((2, spaces - 1)),
        ],
        compiler_params=pltpu.CompilerParams(
            collective_id=0, has_side_effects=True, vmem_limit_bytes=61 * 1024 * 1024
        ),
    )(jnp.asarray(table), *[tiled(a) for a in (sections[0], feed_rate, kill_rate, initial)])
    result = jnp.swapaxes(result, -3, -2).reshape(sections.shape)
    return (result, residual.reshape(()))


def solution(mesh):
    placed = (
        P(None, "space", None),
        P("node", None, "space", None),
        P("space", None),
        P("space", None),
    )
    return jax.shard_map(
        shards,
        mesh=mesh,
        in_specs=placed,
        out_specs=(P("node", None, "space", None), P()),
        check_vma=False,
    )
```

```python
import functools

import jax
import jax.numpy as jnp
import numpy as np
from jax import lax
from jax.experimental import pallas as pl
from jax.experimental.pallas import tpu as pltpu
from jax.sharding import PartitionSpec as P

SWEEPS = 6


step_size = 4.0
diff_u = 1.0
diff_v = 0.5


def radau_target(order, value):
    before = 1.0
    current = value
    previous = 1.0
    for degree in range(1, order):
        following = ((2 * degree + 1) * value * current - degree * before) / (degree + 1)
        before = current
        current = following
    previous = before
    return current - previous


def radau_table(total):
    grid_count = 20000
    roots_found = []
    left_value = -1.0
    left_target = radau_target(total, left_value)
    for step_index in range(1, grid_count):
        right_value = -1.0 + 2.0 * step_index / grid_count
        right_target = radau_target(total, right_value)
        if left_target * right_target < 0.0:
            lower = left_value
            upper = right_value
            lower_target = left_target
            for bisect_index in range(80):
                halfway = 0.5 * (lower + upper)
                halfway_target = radau_target(total, halfway)
                if lower_target * halfway_target <= 0.0:
                    upper = halfway
                else:
                    lower = halfway
                    lower_target = halfway_target
            roots_found.append(0.5 * (lower + upper))
        left_value = right_value
        left_target = right_target
    roots_found.append(1.0)
    points = [(value + 1.0) / 2.0 for value in roots_found]
    quad_rows = []
    for node_index in range(total):
        row_values = []
        for basis_index in range(total):
            coefs = [1.0]
            for other_index in range(total):
                if other_index != basis_index:
                    scale = 1.0 / (points[basis_index] - points[other_index])
                    shifted = [0.0] + coefs
                    widened = coefs + [0.0]
                    coefs = [
                        (shifted[k] - points[other_index] * widened[k]) * scale
                        for k in range(len(shifted))
                    ]
            integral = 0.0
            for power_index in range(len(coefs)):
                integral += (
                    coefs[power_index] * points[node_index] ** (power_index + 1) / (power_index + 1)
                )
            row_values.append(integral)
        quad_rows.append(row_values)
    return (np.array(points), np.array(quad_rows))


MESH = pl.DeviceIdType.MESH
LANES = 128
EDGE = 8
TOP = 2 * EDGE


def kernel(
    nodes,
    spaces,
    table,
    sections,
    feed_rate,
    kill_rate,
    initial,
    out,
    residual,
    sec,
    feed,
    kill,
    init,
    other,
    pack_out,
    pack_in,
    mixed,
    side,
    works_a,
    works_b,
    works_c,
    works_d,
    works_e,
    peak,
    peaks_node,
    peaks_space,
    local_sem,
    halo_sem,
    other_sem,
    pack_sem,
    first_sem,
    second_sem,
    side_sem,
    peak_node_sem,
    peak_space_sem,
):
    works = (works_a, works_b, works_c, works_d, works_e)
    cols = sec.shape[1]
    rows = feed.shape[1]
    block = cols // nodes
    me = lax.axis_index("node")
    here = lax.axis_index("space")
    tall = 2 if nodes % 2 == 0 else 1
    wide = nodes // tall
    chunks = (
        (0, TOP),
        (rows - TOP, TOP),
        (TOP, rows - 5 * EDGE),
        (rows - 3 * EDGE, EDGE),
    )
    pieces = (
        (0, EDGE),
        (rows - EDGE, EDGE),
        (EDGE, rows - 5 * EDGE),
        (rows - 4 * EDGE, 2 * EDGE),
        (rows - 2 * EDGE, EDGE),
    )
    own = me * block

    def moved(m, o):
        return ((m // wide + o // wide) % tall) * wide + (m % wide + o % wide) % wide

    def ahead(o):
        return moved(me, o)

    def negated(o):
        return ((tall - o // wide) % tall) * wide + (wide - o % wide) % wide

    def fetch(source, target, start, size, offset, sem):
        for k in range(start // EDGE, (start + size) // EDGE):
            pltpu.make_async_copy(
                source.at[k], target.at[:, pl.ds(offset + k * EDGE, EDGE)], sem
            ).start()

    def arrived_in(ref, sem):
        pltpu.make_async_copy(ref, ref, sem).wait()

    for i, (start, size) in enumerate(chunks):
        for s in range(2):
            fetch(sections.at[s], sec.at[s], start, size, TOP, local_sem.at[i])

    barrier = pltpu.get_barrier_semaphore()
    for o in range(1, nodes):
        pl.semaphore_signal(barrier, inc=1, device_id={"node": ahead(o)}, device_id_type=MESH)
    for o in range(1, spaces):
        pl.semaphore_signal(
            barrier, inc=1, device_id={"space": (here + o) % spaces}, device_id_type=MESH
        )

    mine = pl.ds(own, block)
    fetch(feed_rate.at[:, mine], feed, 0, rows, 0, local_sem.at[4])
    fetch(kill_rate.at[:, mine], kill, 0, rows, 0, local_sem.at[5])
    for s in range(2):
        fetch(initial.at[s, :, mine], init.at[s], 0, rows, 0, local_sem.at[6])

    def along(ref, sem, way):
        start = TOP + rows - EDGE if way == 0 else TOP
        land = TOP - EDGE if way == 0 else TOP + rows
        target = (here + 1) % spaces if way == 0 else (here + spaces - 1) % spaces
        return pltpu.make_async_remote_copy(
            src_ref=ref.at[:, pl.ds(start, EDGE)],
            dst_ref=ref.at[:, pl.ds(land, EDGE)],
            send_sem=sem.at[0, way],
            recv_sem=sem.at[1, way],
            device_id={"space": target},
            device_id_type=MESH,
        )

    def halo(ref, sem, s, way):
        return along(ref.at[s], sem.at[s], way)

    def forward(o, s, way):
        return along(other.at[o - 1, s, pl.ds(1, block)], other_sem.at[o - 1, s], way)

    def first(p, o):
        start, size = chunks[p]
        where = pl.ds(TOP + start, size)
        return pltpu.make_async_remote_copy(
            src_ref=sec.at[:, pl.ds(ahead(o) * block, block), where],
            dst_ref=other.at[o - 1, :, pl.ds(1, block), where],
            send_sem=first_sem.at[0, p, o - 1],
            recv_sem=first_sem.at[1, p, o - 1],
            device_id={"node": ahead(o)},
            device_id_type=MESH,
        )

    def packed(o):
        return pltpu.make_async_remote_copy(
            src_ref=pack_out.at[o - 1],
            dst_ref=pack_in.at[o - 1],
            send_sem=pack_sem.at[0, o - 1],
            recv_sem=pack_sem.at[1, o - 1],
            device_id={"node": ahead(o)},
            device_id_type=MESH,
        )

    def second(s, p, o):
        start, size = pieces[p]
        return pltpu.make_async_remote_copy(
            src_ref=mixed.at[o - 1, s, :, pl.ds(start, size)],
            dst_ref=side.at[s, mine, pl.ds(TOP + start, size)],
            send_sem=second_sem.at[0, s, p, o - 1],
            recv_sem=second_sem.at[1, s, p, o - 1],
            device_id={"node": ahead(o)},
            device_id_type=MESH,
        )

    order = tuple(range(nodes - 1, 0, -1))
    lane = lax.broadcasted_iota(jnp.int32, (EDGE, LANES), 1)

    def chunk_arrived(i):
        start, size = chunks[i]
        arrived_in(sec.at[:, :, pl.ds(TOP + start, size)], local_sem.at[i])

    chunk_arrived(0)
    chunk_arrived(1)
    pl.semaphore_wait(barrier, nodes - 1 + spaces - 1)
    for p in range(2):
        for o in order:
            first(p, o).start()
    for s in range(2):
        for way in range(2):
            halo(sec, halo_sem, s, way).start()
    chunk_arrived(2)
    chunk_arrived(3)

    groups = rows // EDGE
    for o in order:
        left = (ahead(o) * block + cols - 1) % cols
        right = (ahead(o) * block + block) % cols
        for s in range(2):
            pack = jnp.zeros((EDGE, LANES), jnp.float32)
            for g in range(groups):
                at = pl.ds(TOP + g * EDGE, EDGE)
                both = jnp.where(lane == LANES - 1, sec[s, left, at, :], sec[s, right, at, :])
                pack = jnp.where(lane // 2 == g, pltpu.roll(both, 2 * g + 1, 1), pack)
            pack_out[o - 1, s] = pack
        packed(o).start()
    for p in range(2, 4):
        for o in order:
            first(p, o).start()

    arrived_in(feed, local_sem.at[4])
    arrived_in(kill, local_sem.at[5])
    arrived_in(init, local_sem.at[6])

    for o in order:
        for p in range(2):
            first(p, o).wait_recv()
        for s in range(2):
            for way in range(2):
                forward(o, s, way).start()
    for o in order:
        packed(o).wait_recv()
        for s in range(2):
            pack = pack_in[o - 1, s]
            for g in range(groups):
                at = pl.ds(TOP + g * EDGE, EDGE)
                both = pltpu.roll(pack, LANES - 1 - 2 * g, 1)
                other[o - 1, s, 0, at, :] = both
                other[o - 1, s, block + 1, at, :] = both
    for s in range(2):
        for way in range(2):
            halo(sec, halo_sem, s, way).wait_recv()
    for o in order:
        for s in range(2):
            for way in range(2):
                forward(o, s, way).wait_recv()

    diffs = (diff_u, diff_v)

    def chosen(entries):
        value = jnp.float32(entries[0])
        for m in range(1, nodes):
            value = jnp.where(me == m, jnp.float32(entries[m]), value)
        return value

    every = range(nodes)
    quads, step_table, inverse_table = table
    weights = [
        [chosen([quads[moved(m, t), moved(m, negated(j))] for m in every]) for j in every]
        for t in every
    ]
    steps = [chosen([step_table[moved(m, t)] for m in every]) for t in every]
    inverses = [[chosen([inverse_table[s][moved(m, t)] for m in every]) for t in every] for s in range(2)]

    def ringed(left, middle, right, start):
        at = pl.ds(TOP + start, EDGE)
        here_tile = middle[at, :]
        before = pltpu.roll(jnp.where(lane == LANES - 1, left[at, :], here_tile), 1, 1)
        after = pltpu.roll(jnp.where(lane == 0, right[at, :], here_tile), LANES - 1, 1)
        below = middle[pl.ds(TOP + start + 1, EDGE), :]
        above = middle[pl.ds(TOP + start - 1, EDGE), :]
        return here_tile, (below + above) + (after + before)

    def mix(starts, worst):
        def one(c, worst):
            here_column = own + c
            left = (own + c + cols - 1) % cols
            right = (own + c + 1) % cols
            for start in starts:
                at = pl.ds(start, EDGE)
                f = feed[c, at, :]
                both_rates = f + kill[c, at, :]
                fields, laps, slopes = ([], []), ([], []), ([], [])
                for slot in range(nodes):
                    for s in range(2):
                        if slot == 0:
                            tiles = [sec.at[s, k] for k in (left, here_column, right)]
                        else:
                            tiles = [other.at[slot - 1, s, c + k] for k in range(3)]
                        w, ring = ringed(*tiles, start)
                        fields[s].append(w)
                        laps[s].append(diffs[s] * (ring - 4.0 * w))
                    u, v = fields[0][slot], fields[1][slot]
                    product = u * v * v
                    slopes[0].append(laps[0][slot] + (f * (1.0 - u) - product))
                    slopes[1].append(laps[1][slot] + (product - both_rates * v))
                for s in range(2):
                    base = init[s, c, at, :]
                    for t in range(nodes):
                        to = negated(t)
                        total = weights[t][0] * slopes[s][0]
                        for j in range(1, nodes):
                            total = total + weights[t][j] * slopes[s][j]
                        total = base + total
                        worst = jnp.maximum(worst, jnp.abs(total - fields[s][to]))
                        value = (total - steps[t] * laps[s][to]) * inverses[s][t]
                        if t == 0:
                            side[s, here_column, pl.ds(TOP + start, EDGE), :] = value
                        else:
                            mixed[t - 1, s, c, at, :] = value
            return worst

        return lax.fori_loop(0, block, one, worst)

    def send_back(s, ps):
        for p in ps:
            for o in order:
                second(s, p, o).start()

    def starts_of(ps):
        return [low for p in ps for low in range(pieces[p][0], sum(pieces[p]), EDGE)]

    worst = jnp.zeros((EDGE, LANES), jnp.float32)
    worst = mix(starts_of((0, 1)), worst)
    send_back(0, (0, 1))
    for o in order:
        first(2, o).wait_recv()
    worst = mix(starts_of((2,)), worst)
    send_back(0, (2,))
    for o in order:
        first(3, o).wait_recv()
    worst = mix(starts_of((3, 4)), worst)
    peak[0] = worst

    def peak_node(o):
        return pltpu.make_async_remote_copy(
            src_ref=peak.at[0],
            dst_ref=peaks_node.at[o - 1],
            send_sem=peak_node_sem.at[0, o - 1],
            recv_sem=peak_node_sem.at[1, o - 1],
            device_id={"node": ahead(o)},
            device_id_type=MESH,
        )

    def peak_space(o):
        return pltpu.make_async_remote_copy(
            src_ref=peak.at[1],
            dst_ref=peaks_space.at[o - 1],
            send_sem=peak_space_sem.at[0, o - 1],
            recv_sem=peak_space_sem.at[1, o - 1],
            device_id={"space": (here + o) % spaces},
            device_id_type=MESH,
        )

    for o in range(1, nodes):
        peak_node(o).start()
    send_back(0, (3, 4))
    send_back(1, range(len(pieces)))

    inverse = [inverses[s][0] for s in range(2)]
    factor = [steps[0] * diffs[s] * inverse[s] for s in range(2)]

    def around(ref, s, start, size):
        narrow = lax.broadcasted_iota(jnp.int32, (size, LANES), 1)
        at = pl.ds(start, size)
        tiles = [ref[s, k, at, :] for k in range(cols)]
        sums = []
        for k in range(cols):
            before, tile, after = tiles[k - 1], tiles[k], tiles[(k + 1) % cols]
            left = pltpu.roll(jnp.where(narrow == LANES - 1, before, tile), 1, 1)
            right = pltpu.roll(jnp.where(narrow == 0, after, tile), LANES - 1, 1)
            below = ref[s, k, pl.ds(start + 1, size), :]
            above = ref[s, k, pl.ds(start - 1, size), :]
            sums.append((below + above) + (right + left))
        return sums

    def band(s, spans):
        for k, (start, stop) in enumerate(spans):
            source, plane = (sec, s) if k == 0 else (works[k - 1], 0)
            for low in range(TOP + start, TOP + stop, EDGE):
                size = min(EDGE, TOP + stop - low)
                sums = around(source, plane, low, size)
                for c in range(cols):
                    value = side[s, c, pl.ds(low, size), :] + factor[s] * sums[c]
                    if k == SWEEPS - 1:
                        out[s, (low - TOP) // EDGE, c] = value
                    else:
                        works[k][0, c, pl.ds(low, size), :] = value

    reach = SWEEPS - 1
    cut = rows - 4 * EDGE
    late = rows - 2 * EDGE
    lower = [(k - reach, cut + reach - k - EDGE) for k in range(SWEEPS)]
    middle = [(cut + reach - k - EDGE, late - k) for k in range(reach)] + [(cut - EDGE, cut + EDGE)]
    upper = [(late + EDGE + k, rows + reach - k) for k in range(reach)]
    last = [(late - k, late + EDGE + k) for k in range(reach)] + [(cut + EDGE, rows)]

    def returned(s, p):
        for o in order:
            second(s, p, o).wait_recv()

    for s in range(2):
        returned(s, 0)
        returned(s, 1)
        for way in range(2):
            halo(side, side_sem, s, way).start()
        if s == 0:
            for o in range(1, nodes):
                peak_node(o).wait_recv()
            peak[1] = jnp.maximum(peak[0], jnp.max(peaks_node[...], axis=0))
            for o in range(1, spaces):
                peak_space(o).start()
        returned(s, 2)
        for way in range(2):
            halo(side, side_sem, s, way).wait_recv()
        band(s, lower)
        returned(s, 3)
        band(s, upper)
        band(s, middle)
        if s == 1:
            for o in range(1, spaces):
                peak_space(o).wait_recv()
            residual[...] = jnp.max(
                jnp.maximum(peak[1], jnp.max(peaks_space[...], axis=0)), keepdims=True
            )
        returned(s, 4)
        band(s, last)

    for o in order:
        packed(o).wait_send()
        for p in range(len(chunks)):
            first(p, o).wait_send()
    for s in range(2):
        for way in range(2):
            halo(sec, halo_sem, s, way).wait_send()
            halo(side, side_sem, s, way).wait_send()
            for o in order:
                forward(o, s, way).wait_send()
        for p in range(len(pieces)):
            for o in order:
                second(s, p, o).wait_send()
    for o in range(1, nodes):
        peak_node(o).wait_send()
    for o in range(1, spaces):
        peak_space(o).wait_send()


def shards(initial, sections, feed_rate, kill_rate):
    nodes = lax.axis_size("node")
    spaces = lax.axis_size("space")
    rows, columns = feed_rate.shape
    cols = columns // LANES
    block = cols // nodes
    points, quad_matrix = radau_table(nodes)
    steps = step_size * np.float32(points)
    table = (
        step_size * np.float32(quad_matrix),
        steps,
        [1.0 / (4.0 * (steps * diff) + 1.0) for diff in (diff_u, diff_v)],
    )
    high = TOP + rows + TOP
    f32 = jnp.float32

    def tiled(array):
        split = array.reshape(*array.shape[:-2], rows // EDGE, EDGE, cols, LANES)
        return jnp.swapaxes(split, -3, -2)

    any_spec = pl.BlockSpec(memory_space=pl.ANY)
    dma = pltpu.SemaphoreType.DMA
    result, residual = pl.pallas_call(
        functools.partial(kernel, nodes, spaces, table),
        out_shape=(
            pltpu.VMEM((2, rows // EDGE, cols, EDGE, LANES), f32),
            pltpu.VMEM((1, 1), f32),
        ),
        in_specs=[any_spec] * 4,
        out_specs=(pl.BlockSpec(memory_space=pltpu.VMEM), pl.BlockSpec(memory_space=pltpu.VMEM)),
        scratch_shapes=[
            pltpu.VMEM((2, cols, high, LANES), f32),
            pltpu.VMEM((block, rows, LANES), f32),
            pltpu.VMEM((block, rows, LANES), f32),
            pltpu.VMEM((2, block, rows, LANES), f32),
            pltpu.VMEM((nodes - 1, 2, block + 2, high, LANES), f32),
            pltpu.VMEM((nodes - 1, 2, EDGE, LANES), f32),
            pltpu.VMEM((nodes - 1, 2, EDGE, LANES), f32),
            pltpu.VMEM((nodes - 1, 2, block, rows, LANES), f32),
            pltpu.VMEM((2, cols, high, LANES), f32),
            *[pltpu.VMEM((1, cols, high, LANES), f32)] * (SWEEPS - 1),
            pltpu.VMEM((2, EDGE, LANES), f32),
            pltpu.VMEM((nodes - 1, EDGE, LANES), f32),
            pltpu.VMEM((spaces - 1, EDGE, LANES), f32),
            dma((7,)),
            dma((2, 2, 2)),
            dma((nodes - 1, 2, 2, 2)),
            dma((2, nodes - 1)),
            dma((2, 4, nodes - 1)),
            dma((2, 2, 5, nodes - 1)),
            dma((2, 2, 2)),
            dma((2, nodes - 1)),
            dma((2, spaces - 1)),
        ],
        compiler_params=pltpu.CompilerParams(
            collective_id=0, has_side_effects=True, vmem_limit_bytes=61 * 1024 * 1024
        ),
    )(*[tiled(a) for a in (sections[0], feed_rate, kill_rate, initial)])
    result = jnp.swapaxes(result, -3, -2).reshape(sections.shape)
    return (result, residual.reshape(()))


def solution(mesh):
    placed = (
        P(None, "space", None),
        P("node", None, "space", None),
        P("space", None),
        P("space", None),
    )
    return jax.shard_map(
        shards,
        mesh=mesh,
        in_specs=placed,
        out_specs=(P("node", None, "space", None), P()),
        check_vma=False,
    )
```

```python
import functools

import jax
import jax.numpy as jnp
import numpy as np
from jax import lax
from jax.experimental import pallas as pl
from jax.experimental.pallas import tpu as pltpu
from jax.sharding import PartitionSpec as P

SWEEPS = 6


step_size = 4.0
diff_u = 1.0
diff_v = 0.5


def radau_target(order, value):
    before = 1.0
    current = value
    previous = 1.0
    for degree in range(1, order):
        following = ((2 * degree + 1) * value * current - degree * before) / (degree + 1)
        before = current
        current = following
    previous = before
    return current - previous


def radau_table(total):
    grid_count = 20000
    roots_found = []
    left_value = -1.0
    left_target = radau_target(total, left_value)
    for step_index in range(1, grid_count):
        right_value = -1.0 + 2.0 * step_index / grid_count
        right_target = radau_target(total, right_value)
        if left_target * right_target < 0.0:
            lower = left_value
            upper = right_value
            lower_target = left_target
            for bisect_index in range(80):
                halfway = 0.5 * (lower + upper)
                halfway_target = radau_target(total, halfway)
                if lower_target * halfway_target <= 0.0:
                    upper = halfway
                else:
                    lower = halfway
                    lower_target = halfway_target
            roots_found.append(0.5 * (lower + upper))
        left_value = right_value
        left_target = right_target
    roots_found.append(1.0)
    points = [(value + 1.0) / 2.0 for value in roots_found]
    quad_rows = []
    for node_index in range(total):
        row_values = []
        for basis_index in range(total):
            coefs = [1.0]
            for other_index in range(total):
                if other_index != basis_index:
                    scale = 1.0 / (points[basis_index] - points[other_index])
                    shifted = [0.0] + coefs
                    widened = coefs + [0.0]
                    coefs = [
                        (shifted[k] - points[other_index] * widened[k]) * scale
                        for k in range(len(shifted))
                    ]
            integral = 0.0
            for power_index in range(len(coefs)):
                integral += (
                    coefs[power_index] * points[node_index] ** (power_index + 1) / (power_index + 1)
                )
            row_values.append(integral)
        quad_rows.append(row_values)
    return (np.array(points), np.array(quad_rows))


MESH = pl.DeviceIdType.MESH
LANES = 128
EDGE = 8
TOP = 2 * EDGE


def ringed_sums(ref, s, start, size):
    cols = ref.shape[1]
    narrow = lax.broadcasted_iota(jnp.int32, (size, LANES), 1)
    at = pl.ds(start, size)
    tiles = [ref[s, k, at, :] for k in range(cols)]
    sums = []
    for k in range(cols):
        before, tile, after = tiles[k - 1], tiles[k], tiles[(k + 1) % cols]
        left = pltpu.roll(jnp.where(narrow == LANES - 1, before, tile), 1, 1)
        right = pltpu.roll(jnp.where(narrow == 0, after, tile), LANES - 1, 1)
        below = ref[s, k, pl.ds(start + 1, size), :]
        above = ref[s, k, pl.ds(start - 1, size), :]
        sums.append((below + above) + (right + left))
    return sums


def kernel(
    nodes,
    spaces,
    table,
    sections,
    feed_rate,
    kill_rate,
    initial,
    out,
    worst_out,
    side,
    works_a,
    works_b,
    works_c,
    works_d,
    works_e,
    sec,
    feed,
    kill,
    init,
    other,
    pack_out,
    pack_in,
    mixed,
    peak,
    peaks_node,
    peaks_space,
    local_sem,
    send_sem,
    first_sem,
    second_sem,
    side_sem,
    peak_sem,
    misc_sem,
):
    works = (works_a, works_b, works_c, works_d, works_e)
    cols = sec.shape[1]
    rows = feed.shape[1]
    block = cols // nodes
    me = lax.axis_index("node")
    here = lax.axis_index("space")
    tall = 2 if nodes % 2 == 0 else 1
    wide = nodes // tall
    chunks = (
        (0, TOP),
        (rows - TOP, TOP),
        (TOP, rows - 5 * EDGE),
        (rows - 3 * EDGE, EDGE),
    )
    pieces = (
        (0, EDGE),
        (rows - EDGE, EDGE),
        (EDGE, rows - 5 * EDGE),
        (rows - 4 * EDGE, 2 * EDGE),
        (rows - 2 * EDGE, EDGE),
    )
    own = me * block

    def moved(m, o):
        return ((m // wide + o // wide) % tall) * wide + (m % wide + o % wide) % wide

    def ahead(o):
        return moved(me, o)

    def negated(o):
        return ((tall - o // wide) % tall) * wide + (wide - o % wide) % wide

    def fetch(source, target, start, size, offset, sem):
        for k in range(start // EDGE, (start + size) // EDGE):
            pltpu.make_async_copy(
                source.at[k], target.at[:, pl.ds(offset + k * EDGE, EDGE)], sem
            ).start()

    def arrived_in(ref, sem):
        pltpu.make_async_copy(ref, ref, sem).wait()

    for i, (start, size) in enumerate(chunks):
        for s in range(2):
            fetch(sections.at[s], sec.at[s], start, size, TOP, local_sem.at[i // 2])

    barrier = pltpu.get_barrier_semaphore()
    for o in range(1, nodes):
        pl.semaphore_signal(barrier, inc=1, device_id={"node": ahead(o)}, device_id_type=MESH)
    for o in (1, spaces - 1):
        pl.semaphore_signal(
            barrier, inc=1, device_id={"space": (here + o) % spaces}, device_id_type=MESH
        )

    mine = pl.ds(own, block)
    fetch(feed_rate.at[:, mine], feed, 0, rows, 0, local_sem.at[2])
    fetch(kill_rate.at[:, mine], kill, 0, rows, 0, local_sem.at[2])
    for s in range(2):
        fetch(initial.at[s, :, mine], init.at[s], 0, rows, 0, local_sem.at[3])

    def along(ref, sent, received, way):
        start = TOP + rows - EDGE if way == 0 else TOP
        land = TOP - EDGE if way == 0 else TOP + rows
        target = (here + 1) % spaces if way == 0 else (here + spaces - 1) % spaces
        return pltpu.make_async_remote_copy(
            src_ref=ref.at[:, pl.ds(start, EDGE)],
            dst_ref=ref.at[:, pl.ds(land, EDGE)],
            send_sem=sent,
            recv_sem=received,
            device_id={"space": target},
            device_id_type=MESH,
        )

    def sec_halo(s, way):
        return along(sec.at[s], send_sem.at[0], misc_sem.at[0], way)

    def side_halo(s, way):
        return along(side.at[s], send_sem.at[1], side_sem.at[s], way)

    def forward(o, s, way):
        return along(
            other.at[o - 1, s, pl.ds(1, block)], send_sem.at[2], misc_sem.at[1], way
        )

    def first(p, o):
        start, size = chunks[p]
        where = pl.ds(TOP + start, size)
        return pltpu.make_async_remote_copy(
            src_ref=sec.at[:, pl.ds(ahead(o) * block, block), where],
            dst_ref=other.at[o - 1, :, pl.ds(1, block), where],
            send_sem=send_sem.at[3],
            recv_sem=first_sem.at[max(p - 1, 0)],
            device_id={"node": ahead(o)},
            device_id_type=MESH,
        )

    def packed(o):
        return pltpu.make_async_remote_copy(
            src_ref=pack_out.at[o - 1],
            dst_ref=pack_in.at[o - 1],
            send_sem=send_sem.at[4],
            recv_sem=misc_sem.at[2],
            device_id={"node": ahead(o)},
            device_id_type=MESH,
        )

    def second(s, p, o):
        start, size = pieces[p]
        return pltpu.make_async_remote_copy(
            src_ref=mixed.at[o - 1, s, :, pl.ds(start, size)],
            dst_ref=side.at[s, mine, pl.ds(TOP + start, size)],
            send_sem=send_sem.at[5],
            recv_sem=second_sem.at[s, max(p - 1, 0)],
            device_id={"node": ahead(o)},
            device_id_type=MESH,
        )

    order = tuple(range(nodes - 1, 0, -1))
    lane = lax.broadcasted_iota(jnp.int32, (EDGE, LANES), 1)

    arrived_in(sec.at[:, :, pl.ds(TOP, 2 * TOP)], local_sem.at[0])
    pl.semaphore_wait(barrier, nodes - 1 + 2)
    for p in range(2):
        for o in order:
            first(p, o).start()
    for s in range(2):
        for way in range(2):
            sec_halo(s, way).start()
    arrived_in(sec.at[:, :, pl.ds(TOP, rows - 2 * TOP)], local_sem.at[1])

    groups = rows // EDGE
    for o in order:
        left = (ahead(o) * block + cols - 1) % cols
        right = (ahead(o) * block + block) % cols
        for s in range(2):
            pack = jnp.zeros((EDGE, LANES), jnp.float32)
            for g in range(groups):
                at = pl.ds(TOP + g * EDGE, EDGE)
                both = jnp.where(lane == LANES - 1, sec[s, left, at, :], sec[s, right, at, :])
                pack = jnp.where(lane // 2 == g, pltpu.roll(both, 2 * g + 1, 1), pack)
            pack_out[o - 1, s] = pack
        packed(o).start()
    for p in range(2, 4):
        for o in order:
            first(p, o).start()

    arrived_in(init, local_sem.at[2])
    arrived_in(init, local_sem.at[3])

    def first_arrived(p, size):
        arrived_in(other.at[:, :, pl.ds(1, block), pl.ds(TOP, size)], first_sem.at[p])

    first_arrived(0, 2 * TOP)
    for o in order:
        for s in range(2):
            for way in range(2):
                forward(o, s, way).start()
    arrived_in(pack_in, misc_sem.at[2])
    for o in order:
        for s in range(2):
            pack = pack_in[o - 1, s]
            for g in range(groups):
                at = pl.ds(TOP + g * EDGE, EDGE)
                both = pltpu.roll(pack, LANES - 1 - 2 * g, 1)
                other[o - 1, s, 0, at, :] = both
                other[o - 1, s, block + 1, at, :] = both
    arrived_in(sec.at[:, :, pl.ds(0, 2 * EDGE)], misc_sem.at[0])
    arrived_in(other.at[:, :, pl.ds(1, block), pl.ds(0, 2 * EDGE)], misc_sem.at[1])

    diffs = (diff_u, diff_v)

    def chosen(entries):
        value = jnp.float32(entries[0])
        for m in range(1, nodes):
            value = jnp.where(me == m, jnp.float32(entries[m]), value)
        return value

    every = range(nodes)
    quads, step_table, inverse_table = table
    weights = [
        [chosen([quads[moved(m, t), moved(m, negated(j))] for m in every]) for j in every]
        for t in every
    ]
    steps = [chosen([step_table[moved(m, t)] for m in every]) for t in every]
    inverses = [[chosen([inverse_table[s][moved(m, t)] for m in every]) for t in every] for s in range(2)]

    def ringed(left, middle, right, start):
        at = pl.ds(TOP + start, EDGE)
        here_tile = middle[at, :]
        before = pltpu.roll(jnp.where(lane == LANES - 1, left[at, :], here_tile), 1, 1)
        after = pltpu.roll(jnp.where(lane == 0, right[at, :], here_tile), LANES - 1, 1)
        below = middle[pl.ds(TOP + start + 1, EDGE), :]
        above = middle[pl.ds(TOP + start - 1, EDGE), :]
        return here_tile, (below + above) + (after + before)

    def mix(starts, worst):
        def one(c, worst):
            here_column = own + c
            left = (own + c + cols - 1) % cols
            right = (own + c + 1) % cols
            for start in starts:
                at = pl.ds(start, EDGE)
                f = feed[c, at, :]
                both_rates = f + kill[c, at, :]
                fields, laps, slopes = ([], []), ([], []), ([], [])
                for slot in range(nodes):
                    for s in range(2):
                        if slot == 0:
                            tiles = [sec.at[s, k] for k in (left, here_column, right)]
                        else:
                            tiles = [other.at[slot - 1, s, c + k] for k in range(3)]
                        w, ring = ringed(*tiles, start)
                        fields[s].append(w)
                        laps[s].append(diffs[s] * (ring - 4.0 * w))
                    u, v = fields[0][slot], fields[1][slot]
                    product = u * v * v
                    slopes[0].append(laps[0][slot] + (f * (1.0 - u) - product))
                    slopes[1].append(laps[1][slot] + (product - both_rates * v))
                for s in range(2):
                    base = init[s, c, at, :]
                    for t in range(nodes):
                        to = negated(t)
                        total = weights[t][0] * slopes[s][0]
                        for j in range(1, nodes):
                            total = total + weights[t][j] * slopes[s][j]
                        total = base + total
                        worst = jnp.maximum(worst, jnp.abs(total - fields[s][to]))
                        value = (total - steps[t] * laps[s][to]) * inverses[s][t]
                        if t == 0:
                            side[s, here_column, pl.ds(TOP + start, EDGE), :] = value
                        else:
                            mixed[t - 1, s, c, at, :] = value
            return worst

        return lax.fori_loop(0, block, one, worst)

    def send_back(s, ps):
        for p in ps:
            for o in order:
                second(s, p, o).start()

    def starts_of(ps):
        return [low for p in ps for low in range(pieces[p][0], sum(pieces[p]), EDGE)]

    worst = jnp.zeros((EDGE, LANES), jnp.float32)
    worst = mix(starts_of((0, 1)), worst)
    send_back(0, (0, 1))
    first_arrived(1, chunks[2][1])
    worst = mix(starts_of((2,)), worst)
    send_back(0, (2,))
    first_arrived(2, chunks[3][1])
    worst = mix(starts_of((3, 4)), worst)
    peak[0] = worst

    def peak_node(o):
        return pltpu.make_async_remote_copy(
            src_ref=peak.at[0],
            dst_ref=peaks_node.at[o - 1],
            send_sem=send_sem.at[6],
            recv_sem=misc_sem.at[3],
            device_id={"node": ahead(o)},
            device_id_type=MESH,
        )

    def peak_space(k, way):
        return pltpu.make_async_remote_copy(
            src_ref=peak.at[1 + k],
            dst_ref=peaks_space.at[k, way],
            send_sem=send_sem.at[7],
            recv_sem=peak_sem.at[k],
            device_id={"space": (here + (1, spaces - 1)[way]) % spaces},
            device_id_type=MESH,
        )

    peak_steps = list(range(spaces // 2))
    pace = -(-len(peak_steps) // 4)

    def peak_start(k):
        for way in range(2):
            peak_space(k, way).start()

    def peak_advance():
        for k in peak_steps[:pace]:
            arrived_in(peaks_space.at[k], peak_sem.at[k])
            peak[2 + k] = jnp.maximum(peak[1 + k], jnp.max(peaks_space[k], axis=0))
            if k + 1 < spaces // 2:
                peak_start(k + 1)
        del peak_steps[:pace]

    for o in range(1, nodes):
        peak_node(o).start()
    send_back(0, (3, 4))
    send_back(1, range(len(pieces)))

    inverse = [inverses[s][0] for s in range(2)]
    factor = [steps[0] * diffs[s] * inverse[s] for s in range(2)]

    def put(s, k, low, size, values):
        for c in range(cols):
            if k == SWEEPS - 1:
                out[s, (low - TOP) // EDGE, c] = values[c]
            else:
                works[k][0, c, pl.ds(low, size), :] = values[c]

    def steps_in(span):
        start, stop = span
        return [(low, min(EDGE, TOP + stop - low)) for low in range(TOP + start, TOP + stop, EDGE)]

    def band(s, spans):
        for k, span in enumerate(spans):
            source, plane = (sec, s) if k == 0 else (works[k - 1], 0)
            for low, size in steps_in(span):
                sums = ringed_sums(source, plane, low, size)
                put(s, k, low, size, [
                    side[s, c, pl.ds(low, size), :] + factor[s] * sums[c] for c in range(cols)
                ])

    lower, middle, upper, last = bands_of(rows)

    def returned(s, p, size):
        arrived_in(mixed.at[:, s, :, pl.ds(0, size)], second_sem.at[s, p - 1])

    for s in range(2):
        returned(s, 1, 2 * EDGE)
        for way in range(2):
            side_halo(s, way).start()
        if s == 0:
            arrived_in(peaks_node, misc_sem.at[3])
            peak[1] = jnp.maximum(peak[0], jnp.max(peaks_node[...], axis=0))
            peak_start(0)
        returned(s, 2, pieces[2][1])
        arrived_in(side.at[s, :, pl.ds(0, 2 * EDGE)], side_sem.at[s])
        band(s, lower)
        peak_advance()
        band(s, upper)
        returned(s, 3, pieces[3][1])
        band(s, middle)
        if s == 0:
            peak_advance()
            returned(s, 4, EDGE)
            band(s, last)
            peak_advance()
        else:
            worst_out[...] = jnp.full((EDGE, LANES), jnp.max(peak[1 + spaces // 2]))
            for low, size in steps_in(last[0]):
                sums = ringed_sums(sec, s, low, size)
                put(s, 0, low, size, [factor[s] * total for total in sums])
            returned(s, 4, EDGE)

    arrived_in(sec.at[:, :, pl.ds(0, 2 * EDGE)], send_sem.at[0])
    arrived_in(side.at[:, :, pl.ds(0, 2 * EDGE)], send_sem.at[1])
    arrived_in(other.at[:, :, pl.ds(1, block), pl.ds(0, 2 * EDGE)], send_sem.at[2])
    arrived_in(mixed, send_sem.at[3])
    arrived_in(pack_out, send_sem.at[4])
    arrived_in(mixed, send_sem.at[5])
    arrived_in(peaks_node, send_sem.at[6])
    arrived_in(peaks_space, send_sem.at[7])


def bands_of(rows):
    reach = SWEEPS - 1
    cut = rows - 4 * EDGE
    late = rows - 2 * EDGE
    lower = [(k - reach, cut + reach - k - EDGE) for k in range(SWEEPS)]
    middle = [(cut + reach - k - EDGE, late - k) for k in range(reach)] + [(cut - EDGE, cut + EDGE)]
    upper = [(late + EDGE + k, rows + reach - k) for k in range(reach)]
    last = [(late - k, late + EDGE + k) for k in range(reach)] + [(cut + EDGE, rows)]
    return lower, middle, upper, last


def finish(
    factors,
    swept,
    worst,
    side,
    in_a,
    in_b,
    in_c,
    in_d,
    in_e,
    out,
    residual,
    works_a,
    works_b,
    works_c,
    works_d,
    works_e,
    fresh,
    single,
    sem,
):
    works = (works_a, works_b, works_c, works_d, works_e)
    groups, cols = swept.shape[1:3]
    last = bands_of(groups * EDGE)[3]
    done = last[-1][0] // EDGE
    copies = [
        pltpu.make_async_copy(swept.at[0], out.at[0], sem.at[0]),
        pltpu.make_async_copy(swept.at[1, pl.ds(0, done)], out.at[1, pl.ds(0, done)], sem.at[1]),
        pltpu.make_async_copy(single, residual, sem.at[2]),
    ]
    copies[0].start()
    copies[1].start()
    single[...] = worst[pl.ds(0, 1), pl.ds(0, 1)]
    copies[2].start()
    me = lax.axis_index("node")
    factor = jnp.float32(factors[0])
    for m in range(1, len(factors)):
        factor = jnp.where(me == m, jnp.float32(factors[m]), factor)
    for k, (start, stop) in enumerate(last):
        for low in range(TOP + start, TOP + stop, EDGE):
            size = min(EDGE, TOP + stop - low)
            at = pl.ds(low, size)
            if k == 0:
                for c in range(cols):
                    works[0][0, c, at, :] = works[0][0, c, at, :] + side[1, c, at, :]
                continue
            sums = ringed_sums(works[k - 1], 0, low, size)
            for c in range(cols):
                value = side[1, c, at, :] + factor * sums[c]
                if k == SWEEPS - 1:
                    fresh[(low - TOP) // EDGE - done, c] = value
                else:
                    works[k][0, c, at, :] = value
            if k == SWEEPS - 1:
                g = (low - TOP) // EDGE
                copies.append(
                    pltpu.make_async_copy(fresh.at[g - done], out.at[1, g], sem.at[3 + g - done])
                )
                copies[-1].start()
    for copy in copies:
        copy.wait()


def shards(initial, sections, feed_rate, kill_rate):
    nodes = lax.axis_size("node")
    spaces = lax.axis_size("space")
    rows, columns = feed_rate.shape
    cols = columns // LANES
    block = cols // nodes
    points, quad_matrix = radau_table(nodes)
    steps = step_size * np.float32(points)
    table = (
        step_size * np.float32(quad_matrix),
        steps,
        [1.0 / (4.0 * (steps * diff) + 1.0) for diff in (diff_u, diff_v)],
    )
    high = TOP + rows + TOP
    f32 = jnp.float32
    factors = steps * diff_v * table[2][1]

    def tiled(array):
        split = array.reshape(*array.shape[:-2], rows // EDGE, EDGE, cols, LANES)
        return jnp.swapaxes(split, -3, -2)

    any_spec = pl.BlockSpec(memory_space=pl.ANY)
    dma = pltpu.SemaphoreType.DMA
    vmem = pl.BlockSpec(memory_space=pltpu.VMEM)
    kept = (
        pltpu.VMEM((2, rows // EDGE, cols, EDGE, LANES), f32),
        pltpu.VMEM((EDGE, LANES), f32),
        pltpu.VMEM((2, cols, high, LANES), f32),
        *[pltpu.VMEM((1, cols, high, LANES), f32)] * (SWEEPS - 1),
    )
    room = 64 * 1024 * 1024 - 1024 * 1024 - sum(4 * int(np.prod(a.shape)) for a in kept)
    held = pl.pallas_call(
        functools.partial(kernel, nodes, spaces, table),
        out_shape=kept,
        in_specs=[any_spec] * 4,
        out_specs=(vmem,) * len(kept),
        scratch_shapes=[
            pltpu.VMEM((2, cols, high, LANES), f32),
            pltpu.VMEM((block, rows, LANES), f32),
            pltpu.VMEM((block, rows, LANES), f32),
            pltpu.VMEM((2, block, rows, LANES), f32),
            pltpu.VMEM((nodes - 1, 2, block + 2, high, LANES), f32),
            pltpu.VMEM((nodes - 1, 2, EDGE, LANES), f32),
            pltpu.VMEM((nodes - 1, 2, EDGE, LANES), f32),
            pltpu.VMEM((nodes - 1, 2, block, rows, LANES), f32),
            pltpu.VMEM((2 + spaces // 2, EDGE, LANES), f32),
            pltpu.VMEM((nodes - 1, EDGE, LANES), f32),
            pltpu.VMEM((spaces // 2, 2, EDGE, LANES), f32),
            dma((4,)),
            dma((8,)),
            dma((3,)),
            dma((2, 4)),
            dma((2,)),
            dma((spaces // 2,)),
            dma((4,)),
        ],
        compiler_params=pltpu.CompilerParams(
            collective_id=0, has_side_effects=True, vmem_limit_bytes=room
        ),
    )(*[tiled(a) for a in (sections[0], feed_rate, kill_rate, initial)])
    late = bands_of(rows)[3][-1]
    fresh = (late[1] - late[0]) // EDGE
    result, residual, *_ = pl.pallas_call(
        functools.partial(finish, factors),
        out_shape=(
            jax.ShapeDtypeStruct(kept[0].shape, f32),
            jax.ShapeDtypeStruct((1, 1), f32),
            *kept[3:],
        ),
        in_specs=[vmem] * len(kept),
        out_specs=(any_spec, any_spec, *[vmem] * (SWEEPS - 1)),
        scratch_shapes=[
            pltpu.VMEM((fresh, cols, EDGE, LANES), f32),
            pltpu.VMEM((1, 1), f32),
            dma((3 + fresh,)),
        ],
        input_output_aliases={3 + k: 2 + k for k in range(SWEEPS - 1)},
        compiler_params=pltpu.CompilerParams(vmem_limit_bytes=16 * 1024 * 1024),
    )(*held)
    result = jnp.swapaxes(result, -3, -2).reshape(sections.shape)
    return (result, residual.reshape(()))


def solution(mesh):
    placed = (
        P(None, "space", None),
        P("node", None, "space", None),
        P("space", None),
        P("space", None),
    )
    return jax.shard_map(
        shards,
        mesh=mesh,
        in_specs=placed,
        out_specs=(P("node", None, "space", None), P()),
        check_vma=False,
    )
```

```python
import functools

import jax
import jax.numpy as jnp
import numpy as np
from jax import lax
from jax.experimental import pallas as pl
from jax.experimental.pallas import tpu as pltpu
from jax.sharding import PartitionSpec as P

SWEEPS = 6


step_size = 4.0
diff_u = 1.0
diff_v = 0.5


def radau_target(order, value):
    before = 1.0
    current = value
    previous = 1.0
    for degree in range(1, order):
        following = ((2 * degree + 1) * value * current - degree * before) / (degree + 1)
        before = current
        current = following
    previous = before
    return current - previous


def radau_table(total):
    grid_count = 20000
    roots_found = []
    left_value = -1.0
    left_target = radau_target(total, left_value)
    for step_index in range(1, grid_count):
        right_value = -1.0 + 2.0 * step_index / grid_count
        right_target = radau_target(total, right_value)
        if left_target * right_target < 0.0:
            lower = left_value
            upper = right_value
            lower_target = left_target
            for bisect_index in range(80):
                halfway = 0.5 * (lower + upper)
                halfway_target = radau_target(total, halfway)
                if lower_target * halfway_target <= 0.0:
                    upper = halfway
                else:
                    lower = halfway
                    lower_target = halfway_target
            roots_found.append(0.5 * (lower + upper))
        left_value = right_value
        left_target = right_target
    roots_found.append(1.0)
    points = [(value + 1.0) / 2.0 for value in roots_found]
    quad_rows = []
    for node_index in range(total):
        row_values = []
        for basis_index in range(total):
            coefs = [1.0]
            for other_index in range(total):
                if other_index != basis_index:
                    scale = 1.0 / (points[basis_index] - points[other_index])
                    shifted = [0.0] + coefs
                    widened = coefs + [0.0]
                    coefs = [
                        (shifted[k] - points[other_index] * widened[k]) * scale
                        for k in range(len(shifted))
                    ]
            integral = 0.0
            for power_index in range(len(coefs)):
                integral += (
                    coefs[power_index] * points[node_index] ** (power_index + 1) / (power_index + 1)
                )
            row_values.append(integral)
        quad_rows.append(row_values)
    return (np.array(points), np.array(quad_rows))


MESH = pl.DeviceIdType.MESH
LANES = 128
EDGE = 8
TOP = 2 * EDGE


def ringed_sums(ref, s, start, size):
    cols = ref.shape[1]
    narrow = lax.broadcasted_iota(jnp.int32, (size, LANES), 1)
    at = pl.ds(start, size)
    tiles = [ref[s, k, at, :] for k in range(cols)]
    sums = []
    for k in range(cols):
        before, tile, after = tiles[k - 1], tiles[k], tiles[(k + 1) % cols]
        left = pltpu.roll(jnp.where(narrow == LANES - 1, before, tile), 1, 1)
        right = pltpu.roll(jnp.where(narrow == 0, after, tile), LANES - 1, 1)
        below = ref[s, k, pl.ds(start + 1, size), :]
        above = ref[s, k, pl.ds(start - 1, size), :]
        sums.append((below + above) + (right + left))
    return sums


def kernel(
    nodes,
    spaces,
    table,
    sections,
    feed_rate,
    kill_rate,
    initial,
    out,
    worst_out,
    side,
    works_a,
    works_b,
    works_c,
    works_d,
    works_e,
    sec,
    feed,
    kill,
    init,
    other,
    pack_out,
    pack_in,
    mixed,
    peak,
    peaks_node,
    peaks_space,
    local_sem,
    send_sem,
    first_sem,
    second_sem,
    side_sem,
    peak_sem,
    misc_sem,
):
    works = (works_a, works_b, works_c, works_d, works_e)
    cols = sec.shape[1]
    rows = feed.shape[1]
    block = cols // nodes
    me = lax.axis_index("node")
    here = lax.axis_index("space")
    tall = 2 if nodes % 2 == 0 else 1
    wide = nodes // tall
    chunks = (
        (0, TOP),
        (rows - TOP, TOP),
        (TOP, rows - 5 * EDGE),
        (rows - 3 * EDGE, EDGE),
    )
    pieces = (
        (0, EDGE),
        (rows - EDGE, EDGE),
        (EDGE, rows - 5 * EDGE),
        (rows - 4 * EDGE, 2 * EDGE),
        (rows - 2 * EDGE, EDGE),
    )
    own = me * block

    def moved(m, o):
        return ((m // wide + o // wide) % tall) * wide + (m % wide + o % wide) % wide

    def ahead(o):
        return moved(me, o)

    def negated(o):
        return ((tall - o // wide) % tall) * wide + (wide - o % wide) % wide

    def fetch(source, target, start, size, offset, sem):
        for k in range(start // EDGE, (start + size) // EDGE):
            pltpu.make_async_copy(
                source.at[k], target.at[:, pl.ds(offset + k * EDGE, EDGE)], sem
            ).start()

    def arrived_in(ref, sem):
        pltpu.make_async_copy(ref, ref, sem).wait()

    for i, (start, size) in enumerate(chunks):
        for s in range(2):
            fetch(sections.at[s], sec.at[s], start, size, TOP, local_sem.at[i // 2])

    barrier = pltpu.get_barrier_semaphore()
    for o in range(1, nodes):
        pl.semaphore_signal(barrier, inc=1, device_id={"node": ahead(o)}, device_id_type=MESH)
    for o in (1, spaces - 1):
        pl.semaphore_signal(
            barrier, inc=1, device_id={"space": (here + o) % spaces}, device_id_type=MESH
        )

    mine = pl.ds(own, block)
    fetch(feed_rate.at[:, mine], feed, 0, rows, 0, local_sem.at[2])
    fetch(kill_rate.at[:, mine], kill, 0, rows, 0, local_sem.at[2])
    for s in range(2):
        fetch(initial.at[s, :, mine], init.at[s], 0, rows, 0, local_sem.at[3])

    def along(ref, sent, received, way):
        start = TOP + rows - EDGE if way == 0 else TOP
        land = TOP - EDGE if way == 0 else TOP + rows
        target = (here + 1) % spaces if way == 0 else (here + spaces - 1) % spaces
        return pltpu.make_async_remote_copy(
            src_ref=ref.at[:, pl.ds(start, EDGE)],
            dst_ref=ref.at[:, pl.ds(land, EDGE)],
            send_sem=sent,
            recv_sem=received,
            device_id={"space": target},
            device_id_type=MESH,
        )

    def sec_halo(s, way):
        return along(sec.at[s], send_sem.at[0], misc_sem.at[0], way)

    def side_halo(s, way):
        return along(side.at[s], send_sem.at[1], side_sem.at[s], way)

    def forward(o, s, way):
        return along(
            other.at[o - 1, s, pl.ds(1, block)], send_sem.at[2], misc_sem.at[1], way
        )

    def first(p, o):
        start, size = chunks[p]
        where = pl.ds(TOP + start, size)
        return pltpu.make_async_remote_copy(
            src_ref=sec.at[:, pl.ds(ahead(o) * block, block), where],
            dst_ref=other.at[o - 1, :, pl.ds(1, block), where],
            send_sem=send_sem.at[3],
            recv_sem=first_sem.at[max(p - 1, 0)],
            device_id={"node": ahead(o)},
            device_id_type=MESH,
        )

    def packed(o):
        return pltpu.make_async_remote_copy(
            src_ref=pack_out.at[o - 1],
            dst_ref=pack_in.at[o - 1],
            send_sem=send_sem.at[4],
            recv_sem=misc_sem.at[2],
            device_id={"node": ahead(o)},
            device_id_type=MESH,
        )

    def second(s, p, o):
        start, size = pieces[p]
        return pltpu.make_async_remote_copy(
            src_ref=mixed.at[o - 1, s, :, pl.ds(start, size)],
            dst_ref=side.at[s, mine, pl.ds(TOP + start, size)],
            send_sem=send_sem.at[5],
            recv_sem=second_sem.at[s, max(p - 1, 0)],
            device_id={"node": ahead(o)},
            device_id_type=MESH,
        )

    order = tuple(range(nodes - 1, 0, -1))
    lane = lax.broadcasted_iota(jnp.int32, (EDGE, LANES), 1)

    arrived_in(sec.at[:, :, pl.ds(TOP, 2 * TOP)], local_sem.at[0])
    pl.semaphore_wait(barrier, nodes - 1 + 2)
    for p in range(2):
        for o in order:
            first(p, o).start()
    for s in range(2):
        for way in range(2):
            sec_halo(s, way).start()
    arrived_in(sec.at[:, :, pl.ds(TOP, rows - 2 * TOP)], local_sem.at[1])

    groups = rows // EDGE
    for o in order:
        left = (ahead(o) * block + cols - 1) % cols
        right = (ahead(o) * block + block) % cols
        for s in range(2):
            pack = jnp.zeros((EDGE, LANES), jnp.float32)
            for g in range(groups):
                at = pl.ds(TOP + g * EDGE, EDGE)
                both = jnp.where(lane == LANES - 1, sec[s, left, at, :], sec[s, right, at, :])
                pack = jnp.where(lane // 2 == g, pltpu.roll(both, 2 * g + 1, 1), pack)
            pack_out[o - 1, s] = pack
        packed(o).start()
    for p in range(2, 4):
        for o in order:
            first(p, o).start()

    arrived_in(init, local_sem.at[2])
    arrived_in(init, local_sem.at[3])

    def first_arrived(p, size):
        arrived_in(other.at[:, :, pl.ds(1, block), pl.ds(TOP, size)], first_sem.at[p])

    first_arrived(0, 2 * TOP)
    for o in order:
        for s in range(2):
            for way in range(2):
                forward(o, s, way).start()
    arrived_in(pack_in, misc_sem.at[2])
    for o in order:
        for s in range(2):
            pack = pack_in[o - 1, s]
            for g in range(groups):
                at = pl.ds(TOP + g * EDGE, EDGE)
                both = pltpu.roll(pack, LANES - 1 - 2 * g, 1)
                other[o - 1, s, 0, at, :] = both
                other[o - 1, s, block + 1, at, :] = both
    arrived_in(sec.at[:, :, pl.ds(0, 2 * EDGE)], misc_sem.at[0])
    arrived_in(other.at[:, :, pl.ds(1, block), pl.ds(0, 2 * EDGE)], misc_sem.at[1])

    diffs = (diff_u, diff_v)

    def chosen(entries):
        value = jnp.float32(entries[0])
        for m in range(1, nodes):
            value = jnp.where(me == m, jnp.float32(entries[m]), value)
        return value

    every = range(nodes)
    quads, step_table, inverse_table = table
    weights = [
        [chosen([quads[moved(m, t), moved(m, negated(j))] for m in every]) for j in every]
        for t in every
    ]
    steps = [chosen([step_table[moved(m, t)] for m in every]) for t in every]
    inverses = [[chosen([inverse_table[s][moved(m, t)] for m in every]) for t in every] for s in range(2)]

    def ringed(left, middle, right, start):
        at = pl.ds(TOP + start, EDGE)
        here_tile = middle[at, :]
        before = pltpu.roll(jnp.where(lane == LANES - 1, left[at, :], here_tile), 1, 1)
        after = pltpu.roll(jnp.where(lane == 0, right[at, :], here_tile), LANES - 1, 1)
        below = middle[pl.ds(TOP + start + 1, EDGE), :]
        above = middle[pl.ds(TOP + start - 1, EDGE), :]
        return here_tile, (below + above) + (after + before)

    def mix(starts, worst):
        def one(c, worst):
            here_column = own + c
            left = (own + c + cols - 1) % cols
            right = (own + c + 1) % cols
            for start in starts:
                at = pl.ds(start, EDGE)
                f = feed[c, at, :]
                both_rates = f + kill[c, at, :]
                fields, laps, slopes = ([], []), ([], []), ([], [])
                for slot in range(nodes):
                    for s in range(2):
                        if slot == 0:
                            tiles = [sec.at[s, k] for k in (left, here_column, right)]
                        else:
                            tiles = [other.at[slot - 1, s, c + k] for k in range(3)]
                        w, ring = ringed(*tiles, start)
                        fields[s].append(w)
                        laps[s].append(diffs[s] * (ring - 4.0 * w))
                    u, v = fields[0][slot], fields[1][slot]
                    product = u * v * v
                    slopes[0].append(laps[0][slot] + (f * (1.0 - u) - product))
                    slopes[1].append(laps[1][slot] + (product - both_rates * v))
                for s in range(2):
                    base = init[s, c, at, :]
                    for t in range(nodes):
                        to = negated(t)
                        total = weights[t][0] * slopes[s][0]
                        for j in range(1, nodes):
                            total = total + weights[t][j] * slopes[s][j]
                        total = base + total
                        worst = jnp.maximum(worst, jnp.abs(total - fields[s][to]))
                        value = (total - steps[t] * laps[s][to]) * inverses[s][t]
                        if t == 0:
                            side[s, here_column, pl.ds(TOP + start, EDGE), :] = value
                        else:
                            mixed[t - 1, s, c, at, :] = value
            return worst

        return lax.fori_loop(0, block, one, worst)

    def send_back(s, ps):
        for p in ps:
            for o in order:
                second(s, p, o).start()

    def starts_of(ps):
        return [low for p in ps for low in range(pieces[p][0], sum(pieces[p]), EDGE)]

    worst = jnp.zeros((EDGE, LANES), jnp.float32)
    worst = mix(starts_of((0, 1)), worst)
    send_back(0, (0, 1))
    first_arrived(1, chunks[2][1])
    worst = mix(starts_of((2,)), worst)
    send_back(0, (2,))
    first_arrived(2, chunks[3][1])
    worst = mix(starts_of((3, 4)), worst)
    peak[0] = worst

    def peak_node(o):
        return pltpu.make_async_remote_copy(
            src_ref=peak.at[0],
            dst_ref=peaks_node.at[o - 1],
            send_sem=send_sem.at[6],
            recv_sem=misc_sem.at[3],
            device_id={"node": ahead(o)},
            device_id_type=MESH,
        )

    def peak_space(k):
        apart = 2**k
        return pltpu.make_async_remote_copy(
            src_ref=peak.at[1 + k],
            dst_ref=peaks_space.at[k],
            send_sem=send_sem.at[7],
            recv_sem=peak_sem.at[k],
            device_id={"space": here + apart - here // apart % 2 * 2 * apart},
            device_id_type=MESH,
        )

    doublings = peaks_space.shape[0]
    peak_steps = list(range(doublings))
    pace = -(-doublings // 3)

    def peak_advance():
        for k in peak_steps[:pace]:
            arrived_in(peaks_space.at[k], peak_sem.at[k])
            peak[2 + k] = jnp.maximum(peak[1 + k], peaks_space[k])
            if k + 1 < doublings:
                peak_space(k + 1).start()
        del peak_steps[:pace]

    for o in range(1, nodes):
        peak_node(o).start()
    send_back(0, (3, 4))
    send_back(1, range(len(pieces)))

    inverse = [inverses[s][0] for s in range(2)]
    factor = [steps[0] * diffs[s] * inverse[s] for s in range(2)]

    def put(s, k, low, size, values):
        for c in range(cols):
            if k == SWEEPS - 1:
                out[s, (low - TOP) // EDGE, c] = values[c]
            else:
                works[k][0, c, pl.ds(low, size), :] = values[c]

    def steps_in(span):
        start, stop = span
        return [(low, min(EDGE, TOP + stop - low)) for low in range(TOP + start, TOP + stop, EDGE)]

    def band(s, spans):
        for k, span in enumerate(spans):
            source, plane = (sec, s) if k == 0 else (works[k - 1], 0)
            for low, size in steps_in(span):
                sums = ringed_sums(source, plane, low, size)
                put(s, k, low, size, [
                    side[s, c, pl.ds(low, size), :] + factor[s] * sums[c] for c in range(cols)
                ])

    lower, middle, upper, last = bands_of(rows)

    def returned(s, p, size):
        arrived_in(mixed.at[:, s, :, pl.ds(0, size)], second_sem.at[s, p - 1])

    for s in range(2):
        returned(s, 1, 2 * EDGE)
        for way in range(2):
            side_halo(s, way).start()
        if s == 0:
            arrived_in(peaks_node, misc_sem.at[3])
            peak[1] = jnp.maximum(peak[0], jnp.max(peaks_node[...], axis=0))
            peak_space(0).start()
        else:
            peak_advance()
            worst_out[...] = jnp.full((EDGE, LANES), jnp.max(peak[1 + doublings]))
        returned(s, 2, pieces[2][1])
        arrived_in(side.at[s, :, pl.ds(0, 2 * EDGE)], side_sem.at[s])
        band(s, lower)
        if s == 0:
            peak_advance()
        band(s, upper)
        returned(s, 3, pieces[3][1])
        band(s, middle)
        if s == 0:
            peak_advance()
            returned(s, 4, EDGE)
            band(s, last)
        else:
            for low, size in steps_in(last[0]):
                sums = ringed_sums(sec, s, low, size)
                put(s, 0, low, size, [factor[s] * total for total in sums])
            returned(s, 4, EDGE)

    arrived_in(sec.at[:, :, pl.ds(0, 2 * EDGE)], send_sem.at[0])
    arrived_in(side.at[:, :, pl.ds(0, 2 * EDGE)], send_sem.at[1])
    arrived_in(other.at[:, :, pl.ds(1, block), pl.ds(0, 2 * EDGE)], send_sem.at[2])
    arrived_in(mixed, send_sem.at[3])
    arrived_in(pack_out, send_sem.at[4])
    arrived_in(mixed, send_sem.at[5])
    arrived_in(peaks_node, send_sem.at[6])
    arrived_in(peaks_space, send_sem.at[7])


def bands_of(rows):
    reach = SWEEPS - 1
    cut = rows - 4 * EDGE
    late = rows - 2 * EDGE
    lower = [(k - reach, cut + reach - k - EDGE) for k in range(SWEEPS)]
    middle = [(cut + reach - k - EDGE, late - k) for k in range(reach)] + [(cut - EDGE, cut + EDGE)]
    upper = [(late + EDGE + k, rows + reach - k) for k in range(reach)]
    last = [(late - k, late + EDGE + k) for k in range(reach)] + [(cut + EDGE, rows)]
    return lower, middle, upper, last


def finish(
    factors,
    swept,
    worst,
    side,
    in_a,
    in_b,
    in_c,
    in_d,
    in_e,
    out,
    residual,
    works_a,
    works_b,
    works_c,
    works_d,
    works_e,
    fresh,
    single,
    sem,
):
    works = (works_a, works_b, works_c, works_d, works_e)
    groups, cols = swept.shape[1:3]
    last = bands_of(groups * EDGE)[3]
    done = last[-1][0] // EDGE
    copies = [
        pltpu.make_async_copy(swept.at[0], out.at[0], sem.at[0]),
        pltpu.make_async_copy(swept.at[1, pl.ds(0, done)], out.at[1, pl.ds(0, done)], sem.at[1]),
        pltpu.make_async_copy(single, residual, sem.at[2]),
    ]
    copies[0].start()
    copies[1].start()
    single[...] = worst[pl.ds(0, 1), pl.ds(0, 1)]
    copies[2].start()
    me = lax.axis_index("node")
    factor = jnp.float32(factors[0])
    for m in range(1, len(factors)):
        factor = jnp.where(me == m, jnp.float32(factors[m]), factor)
    for k, (start, stop) in enumerate(last):
        for low in range(TOP + start, TOP + stop, EDGE):
            size = min(EDGE, TOP + stop - low)
            at = pl.ds(low, size)
            if k == 0:
                for c in range(cols):
                    works[0][0, c, at, :] = works[0][0, c, at, :] + side[1, c, at, :]
                continue
            sums = ringed_sums(works[k - 1], 0, low, size)
            for c in range(cols):
                value = side[1, c, at, :] + factor * sums[c]
                if k == SWEEPS - 1:
                    fresh[(low - TOP) // EDGE - done, c] = value
                else:
                    works[k][0, c, at, :] = value
            if k == SWEEPS - 1:
                g = (low - TOP) // EDGE
                copies.append(
                    pltpu.make_async_copy(fresh.at[g - done], out.at[1, g], sem.at[3 + g - done])
                )
                copies[-1].start()
    for copy in copies:
        copy.wait()


def shards(initial, sections, feed_rate, kill_rate):
    nodes = lax.axis_size("node")
    spaces = lax.axis_size("space")
    rows, columns = feed_rate.shape
    cols = columns // LANES
    block = cols // nodes
    doublings = (spaces - 1).bit_length()
    points, quad_matrix = radau_table(nodes)
    steps = step_size * np.float32(points)
    table = (
        step_size * np.float32(quad_matrix),
        steps,
        [1.0 / (4.0 * (steps * diff) + 1.0) for diff in (diff_u, diff_v)],
    )
    high = TOP + rows + TOP
    f32 = jnp.float32
    factors = steps * diff_v * table[2][1]

    def tiled(array):
        split = array.reshape(*array.shape[:-2], rows // EDGE, EDGE, cols, LANES)
        return jnp.swapaxes(split, -3, -2)

    any_spec = pl.BlockSpec(memory_space=pl.ANY)
    dma = pltpu.SemaphoreType.DMA
    vmem = pl.BlockSpec(memory_space=pltpu.VMEM)
    kept = (
        pltpu.VMEM((2, rows // EDGE, cols, EDGE, LANES), f32),
        pltpu.VMEM((EDGE, LANES), f32),
        pltpu.VMEM((2, cols, high, LANES), f32),
        *[pltpu.VMEM((1, cols, high, LANES), f32)] * (SWEEPS - 1),
    )
    room = 64 * 1024 * 1024 - 1024 * 1024 - sum(4 * int(np.prod(a.shape)) for a in kept)
    held = pl.pallas_call(
        functools.partial(kernel, nodes, spaces, table),
        out_shape=kept,
        in_specs=[any_spec] * 4,
        out_specs=(vmem,) * len(kept),
        scratch_shapes=[
            pltpu.VMEM((2, cols, high, LANES), f32),
            pltpu.VMEM((block, rows, LANES), f32),
            pltpu.VMEM((block, rows, LANES), f32),
            pltpu.VMEM((2, block, rows, LANES), f32),
            pltpu.VMEM((nodes - 1, 2, block + 2, high, LANES), f32),
            pltpu.VMEM((nodes - 1, 2, EDGE, LANES), f32),
            pltpu.VMEM((nodes - 1, 2, EDGE, LANES), f32),
            pltpu.VMEM((nodes - 1, 2, block, rows, LANES), f32),
            pltpu.VMEM((2 + doublings, EDGE, LANES), f32),
            pltpu.VMEM((nodes - 1, EDGE, LANES), f32),
            pltpu.VMEM((doublings, EDGE, LANES), f32),
            dma((4,)),
            dma((8,)),
            dma((3,)),
            dma((2, 4)),
            dma((2,)),
            dma((doublings,)),
            dma((4,)),
        ],
        compiler_params=pltpu.CompilerParams(
            collective_id=0, has_side_effects=True, vmem_limit_bytes=room
        ),
    )(*[tiled(a) for a in (sections[0], feed_rate, kill_rate, initial)])
    late = bands_of(rows)[3][-1]
    fresh = (late[1] - late[0]) // EDGE
    result, residual, *_ = pl.pallas_call(
        functools.partial(finish, factors),
        out_shape=(
            jax.ShapeDtypeStruct(kept[0].shape, f32),
            jax.ShapeDtypeStruct((1, 1), f32),
            *kept[3:],
        ),
        in_specs=[vmem] * len(kept),
        out_specs=(any_spec, any_spec, *[vmem] * (SWEEPS - 1)),
        scratch_shapes=[
            pltpu.VMEM((fresh, cols, EDGE, LANES), f32),
            pltpu.VMEM((1, 1), f32),
            dma((3 + fresh,)),
        ],
        input_output_aliases={3 + k: 2 + k for k in range(SWEEPS - 1)},
        compiler_params=pltpu.CompilerParams(vmem_limit_bytes=16 * 1024 * 1024),
    )(*held)
    result = jnp.swapaxes(result, -3, -2).reshape(sections.shape)
    return (result, residual.reshape(()))


def solution(mesh):
    placed = (
        P(None, "space", None),
        P("node", None, "space", None),
        P("space", None),
        P("space", None),
    )
    return jax.shard_map(
        shards,
        mesh=mesh,
        in_specs=placed,
        out_specs=(P("node", None, "space", None), P()),
        check_vma=False,
    )
```

```python
import functools

import jax
import jax.numpy as jnp
import numpy as np
from jax import lax
from jax.experimental import pallas as pl
from jax.experimental.pallas import tpu as pltpu
from jax.sharding import PartitionSpec as P

SWEEPS = 6


step_size = 4.0
diff_u = 1.0
diff_v = 0.5


def radau_target(order, value):
    before = 1.0
    current = value
    previous = 1.0
    for degree in range(1, order):
        following = ((2 * degree + 1) * value * current - degree * before) / (degree + 1)
        before = current
        current = following
    previous = before
    return current - previous


def radau_table(total):
    grid_count = 20000
    roots_found = []
    left_value = -1.0
    left_target = radau_target(total, left_value)
    for step_index in range(1, grid_count):
        right_value = -1.0 + 2.0 * step_index / grid_count
        right_target = radau_target(total, right_value)
        if left_target * right_target < 0.0:
            lower = left_value
            upper = right_value
            lower_target = left_target
            for bisect_index in range(80):
                halfway = 0.5 * (lower + upper)
                halfway_target = radau_target(total, halfway)
                if lower_target * halfway_target <= 0.0:
                    upper = halfway
                else:
                    lower = halfway
                    lower_target = halfway_target
            roots_found.append(0.5 * (lower + upper))
        left_value = right_value
        left_target = right_target
    roots_found.append(1.0)
    points = [(value + 1.0) / 2.0 for value in roots_found]
    quad_rows = []
    for node_index in range(total):
        row_values = []
        for basis_index in range(total):
            coefs = [1.0]
            for other_index in range(total):
                if other_index != basis_index:
                    scale = 1.0 / (points[basis_index] - points[other_index])
                    shifted = [0.0] + coefs
                    widened = coefs + [0.0]
                    coefs = [
                        (shifted[k] - points[other_index] * widened[k]) * scale
                        for k in range(len(shifted))
                    ]
            integral = 0.0
            for power_index in range(len(coefs)):
                integral += (
                    coefs[power_index] * points[node_index] ** (power_index + 1) / (power_index + 1)
                )
            row_values.append(integral)
        quad_rows.append(row_values)
    return (np.array(points), np.array(quad_rows))


MESH = pl.DeviceIdType.MESH
LANES = 128
EDGE = 8
TOP = 2 * EDGE


def ringed_sums(ref, s, start, size):
    cols = ref.shape[1]
    narrow = lax.broadcasted_iota(jnp.int32, (size, LANES), 1)
    at = pl.ds(start, size)
    tiles = [ref[s, k, at, :] for k in range(cols)]
    sums = []
    for k in range(cols):
        before, tile, after = tiles[k - 1], tiles[k], tiles[(k + 1) % cols]
        left = pltpu.roll(jnp.where(narrow == LANES - 1, before, tile), 1, 1)
        right = pltpu.roll(jnp.where(narrow == 0, after, tile), LANES - 1, 1)
        below = ref[s, k, pl.ds(start + 1, size), :]
        above = ref[s, k, pl.ds(start - 1, size), :]
        sums.append((below + above) + (right + left))
    return sums


def kernel(
    nodes,
    spaces,
    table,
    sections,
    feed_rate,
    kill_rate,
    initial,
    out,
    worst_out,
    side,
    works_a,
    works_b,
    works_c,
    works_d,
    works_e,
    sec,
    feed,
    kill,
    init,
    other,
    pack_out,
    pack_in,
    mixed,
    peak,
    peaks_node,
    peaks_space,
    local_sem,
    send_sem,
    first_sem,
    second_sem,
    side_sem,
    peak_sem,
    misc_sem,
):
    works = (works_a, works_b, works_c, works_d, works_e)
    cols = sec.shape[1]
    rows = feed.shape[1]
    block = cols // nodes
    me = lax.axis_index("node")
    here = lax.axis_index("space")
    tall = 2 if nodes % 2 == 0 else 1
    wide = nodes // tall
    chunks = (
        (0, TOP),
        (rows - TOP, TOP),
        (TOP, rows - 5 * EDGE),
        (rows - 3 * EDGE, EDGE),
    )
    pieces = (
        (0, EDGE),
        (rows - EDGE, EDGE),
        (EDGE, rows - 5 * EDGE),
        (rows - 4 * EDGE, 2 * EDGE),
        (rows - 2 * EDGE, EDGE),
    )
    own = me * block

    def moved(m, o):
        return ((m // wide + o // wide) % tall) * wide + (m % wide + o % wide) % wide

    def ahead(o):
        return moved(me, o)

    def negated(o):
        return ((tall - o // wide) % tall) * wide + (wide - o % wide) % wide

    def fetch(source, target, start, size, offset, sem):
        for k in range(start // EDGE, (start + size) // EDGE):
            pltpu.make_async_copy(
                source.at[k], target.at[:, pl.ds(offset + k * EDGE, EDGE)], sem
            ).start()

    def arrived_in(ref, sem):
        pltpu.make_async_copy(ref, ref, sem).wait()

    for i, (start, size) in enumerate(chunks):
        for s in range(2):
            fetch(sections.at[s], sec.at[s], start, size, TOP, local_sem.at[i // 2])

    barrier = pltpu.get_barrier_semaphore()
    for o in range(1, nodes):
        pl.semaphore_signal(barrier, inc=1, device_id={"node": ahead(o)}, device_id_type=MESH)
    for o in (1, spaces - 1):
        pl.semaphore_signal(
            barrier, inc=1, device_id={"space": (here + o) % spaces}, device_id_type=MESH
        )

    mine = pl.ds(own, block)
    fetch(feed_rate.at[:, mine], feed, 0, rows, 0, local_sem.at[2])
    fetch(kill_rate.at[:, mine], kill, 0, rows, 0, local_sem.at[2])
    for s in range(2):
        fetch(initial.at[s, :, mine], init.at[s], 0, rows, 0, local_sem.at[3])

    def along(ref, sent, received, way):
        start = TOP + rows - EDGE if way == 0 else TOP
        land = TOP - EDGE if way == 0 else TOP + rows
        target = (here + 1) % spaces if way == 0 else (here + spaces - 1) % spaces
        return pltpu.make_async_remote_copy(
            src_ref=ref.at[:, pl.ds(start, EDGE)],
            dst_ref=ref.at[:, pl.ds(land, EDGE)],
            send_sem=sent,
            recv_sem=received,
            device_id={"space": target},
            device_id_type=MESH,
        )

    def sec_halo(s, way):
        return along(sec.at[s], send_sem.at[0], misc_sem.at[0], way)

    def side_halo(s, way):
        return along(side.at[s], send_sem.at[1], side_sem.at[s], way)

    def forward(o, s, way):
        return along(
            other.at[o - 1, s, pl.ds(1, block)], send_sem.at[2], misc_sem.at[1], way
        )

    def first(p, o):
        start, size = chunks[p]
        where = pl.ds(TOP + start, size)
        return pltpu.make_async_remote_copy(
            src_ref=sec.at[:, pl.ds(ahead(o) * block, block), where],
            dst_ref=other.at[o - 1, :, pl.ds(1, block), where],
            send_sem=send_sem.at[3],
            recv_sem=first_sem.at[max(p - 1, 0)],
            device_id={"node": ahead(o)},
            device_id_type=MESH,
        )

    def packed(o):
        return pltpu.make_async_remote_copy(
            src_ref=pack_out.at[o - 1],
            dst_ref=pack_in.at[o - 1],
            send_sem=send_sem.at[4],
            recv_sem=misc_sem.at[2],
            device_id={"node": ahead(o)},
            device_id_type=MESH,
        )

    def second(s, p, o):
        start, size = pieces[p]
        return pltpu.make_async_remote_copy(
            src_ref=mixed.at[o - 1, s, :, pl.ds(start, size)],
            dst_ref=side.at[s, mine, pl.ds(TOP + start, size)],
            send_sem=send_sem.at[5],
            recv_sem=second_sem.at[s, max(p - 1, 0)],
            device_id={"node": ahead(o)},
            device_id_type=MESH,
        )

    order = tuple(range(nodes - 1, 0, -1))
    lane = lax.broadcasted_iota(jnp.int32, (EDGE, LANES), 1)

    arrived_in(sec.at[:, :, pl.ds(TOP, 2 * TOP)], local_sem.at[0])
    pl.semaphore_wait(barrier, nodes - 1 + 2)
    for p in range(2):
        for o in order:
            first(p, o).start()
    for s in range(2):
        for way in range(2):
            sec_halo(s, way).start()
    arrived_in(sec.at[:, :, pl.ds(TOP, rows - 2 * TOP)], local_sem.at[1])

    groups = rows // EDGE
    for o in order:
        left = (ahead(o) * block + cols - 1) % cols
        right = (ahead(o) * block + block) % cols
        for s in range(2):
            pack = jnp.zeros((EDGE, LANES), jnp.float32)
            for g in range(groups):
                at = pl.ds(TOP + g * EDGE, EDGE)
                both = jnp.where(lane == LANES - 1, sec[s, left, at, :], sec[s, right, at, :])
                pack = jnp.where(lane // 2 == g, pltpu.roll(both, 2 * g + 1, 1), pack)
            pack_out[o - 1, s] = pack
        packed(o).start()
    for p in range(2, 4):
        for o in order:
            first(p, o).start()

    arrived_in(init, local_sem.at[2])
    arrived_in(init, local_sem.at[3])

    def first_arrived(p, size):
        arrived_in(other.at[:, :, pl.ds(1, block), pl.ds(TOP, size)], first_sem.at[p])

    first_arrived(0, 2 * TOP)
    for o in order:
        for s in range(2):
            for way in range(2):
                forward(o, s, way).start()
    arrived_in(pack_in, misc_sem.at[2])
    for o in order:
        for s in range(2):
            pack = pack_in[o - 1, s]
            for g in range(groups):
                at = pl.ds(TOP + g * EDGE, EDGE)
                both = pltpu.roll(pack, LANES - 1 - 2 * g, 1)
                other[o - 1, s, 0, at, :] = both
                other[o - 1, s, block + 1, at, :] = both
    arrived_in(sec.at[:, :, pl.ds(0, 2 * EDGE)], misc_sem.at[0])
    arrived_in(other.at[:, :, pl.ds(1, block), pl.ds(0, 2 * EDGE)], misc_sem.at[1])

    diffs = (diff_u, diff_v)

    def chosen(entries):
        value = jnp.float32(entries[0])
        for m in range(1, nodes):
            value = jnp.where(me == m, jnp.float32(entries[m]), value)
        return value

    every = range(nodes)
    quads, step_table, inverse_table = table
    weights = [
        [chosen([quads[moved(m, t), moved(m, negated(j))] for m in every]) for j in every]
        for t in every
    ]
    steps = [chosen([step_table[moved(m, t)] for m in every]) for t in every]
    inverses = [[chosen([inverse_table[s][moved(m, t)] for m in every]) for t in every] for s in range(2)]

    def ringed(left, middle, right, start):
        at = pl.ds(TOP + start, EDGE)
        here_tile = middle[at, :]
        before = pltpu.roll(jnp.where(lane == LANES - 1, left[at, :], here_tile), 1, 1)
        after = pltpu.roll(jnp.where(lane == 0, right[at, :], here_tile), LANES - 1, 1)
        below = middle[pl.ds(TOP + start + 1, EDGE), :]
        above = middle[pl.ds(TOP + start - 1, EDGE), :]
        return here_tile, (below + above) + (after + before)

    def mix(starts, worst):
        def one(c, worst):
            here_column = own + c
            left = (own + c + cols - 1) % cols
            right = (own + c + 1) % cols
            for start in starts:
                at = pl.ds(start, EDGE)
                f = feed[c, at, :]
                both_rates = f + kill[c, at, :]
                fields, laps, slopes = ([], []), ([], []), ([], [])
                for slot in range(nodes):
                    for s in range(2):
                        if slot == 0:
                            tiles = [sec.at[s, k] for k in (left, here_column, right)]
                        else:
                            tiles = [other.at[slot - 1, s, c + k] for k in range(3)]
                        w, ring = ringed(*tiles, start)
                        fields[s].append(w)
                        laps[s].append(diffs[s] * (ring - 4.0 * w))
                    u, v = fields[0][slot], fields[1][slot]
                    product = u * v * v
                    slopes[0].append(laps[0][slot] + (f * (1.0 - u) - product))
                    slopes[1].append(laps[1][slot] + (product - both_rates * v))
                for s in range(2):
                    base = init[s, c, at, :]
                    for t in range(nodes):
                        to = negated(t)
                        total = weights[t][0] * slopes[s][0]
                        for j in range(1, nodes):
                            total = total + weights[t][j] * slopes[s][j]
                        total = base + total
                        worst = jnp.maximum(worst, jnp.abs(total - fields[s][to]))
                        value = (total - steps[t] * laps[s][to]) * inverses[s][t]
                        if t == 0:
                            side[s, here_column, pl.ds(TOP + start, EDGE), :] = value
                        else:
                            mixed[t - 1, s, c, at, :] = value
            return worst

        return lax.fori_loop(0, block, one, worst)

    def send_back(s, ps):
        for p in ps:
            for o in order:
                second(s, p, o).start()

    def starts_of(ps):
        return [low for p in ps for low in range(pieces[p][0], sum(pieces[p]), EDGE)]

    worst = jnp.zeros((EDGE, LANES), jnp.float32)
    worst = mix(starts_of((0, 1)), worst)
    send_back(0, (0, 1))
    send_back(1, (0, 1))
    first_arrived(1, chunks[2][1])
    worst = mix(starts_of((2,)), worst)
    send_back(0, (2,))
    first_arrived(2, chunks[3][1])
    worst = mix(starts_of((3, 4)), worst)
    peak[0] = worst

    def peak_node(o):
        return pltpu.make_async_remote_copy(
            src_ref=peak.at[0],
            dst_ref=peaks_node.at[o - 1],
            send_sem=send_sem.at[6],
            recv_sem=misc_sem.at[3],
            device_id={"node": ahead(o)},
            device_id_type=MESH,
        )

    def peak_space(k):
        apart = 2**k
        return pltpu.make_async_remote_copy(
            src_ref=peak.at[1 + k],
            dst_ref=peaks_space.at[k],
            send_sem=send_sem.at[7],
            recv_sem=peak_sem.at[k],
            device_id={"space": here + apart - here // apart % 2 * 2 * apart},
            device_id_type=MESH,
        )

    doublings = peaks_space.shape[0]
    peak_steps = list(range(doublings))
    pace = -(-doublings // 3)

    def peak_advance():
        for k in peak_steps[:pace]:
            arrived_in(peaks_space.at[k], peak_sem.at[k])
            peak[2 + k] = jnp.maximum(peak[1 + k], peaks_space[k])
            if k + 1 < doublings:
                peak_space(k + 1).start()
        del peak_steps[:pace]

    for o in range(1, nodes):
        peak_node(o).start()
    send_back(0, (3, 4))
    send_back(1, (2, 3, 4))

    inverse = [inverses[s][0] for s in range(2)]
    factor = [steps[0] * diffs[s] * inverse[s] for s in range(2)]

    def put(s, k, low, size, values):
        for c in range(cols):
            if k == SWEEPS - 1:
                out[s, (low - TOP) // EDGE, c] = values[c]
            else:
                works[k][0, c, pl.ds(low, size), :] = values[c]

    def steps_in(span):
        start, stop = span
        return [(low, min(EDGE, TOP + stop - low)) for low in range(TOP + start, TOP + stop, EDGE)]

    def band(s, spans):
        for k, span in enumerate(spans):
            source, plane = (sec, s) if k == 0 else (works[k - 1], 0)
            for low, size in steps_in(span):
                sums = ringed_sums(source, plane, low, size)
                put(s, k, low, size, [
                    side[s, c, pl.ds(low, size), :] + factor[s] * sums[c] for c in range(cols)
                ])

    lower, middle, upper, last = bands_of(rows)

    def returned(s, p, size):
        arrived_in(mixed.at[:, s, :, pl.ds(0, size)], second_sem.at[s, p - 1])

    for s in range(2):
        returned(s, 1, 2 * EDGE)
        for way in range(2):
            side_halo(s, way).start()

    for s in range(2):
        arrived_in(side.at[s, :, pl.ds(0, 2 * EDGE)], side_sem.at[s])
        band(s, upper)
        if s == 1:
            peak_advance()
        returned(s, 2, pieces[2][1])
        band(s, lower)
        if s == 0:
            arrived_in(peaks_node, misc_sem.at[3])
            peak[1] = jnp.maximum(peak[0], jnp.max(peaks_node[...], axis=0))
            peak_space(0).start()
        else:
            peak_advance()
            worst_out[...] = jnp.full((EDGE, LANES), jnp.max(peak[1 + doublings]))
        returned(s, 3, pieces[3][1])
        band(s, middle)
        if s == 0:
            peak_advance()
            returned(s, 4, EDGE)
            band(s, last)
        else:
            for low, size in steps_in(last[0]):
                sums = ringed_sums(sec, s, low, size)
                put(s, 0, low, size, [factor[s] * total for total in sums])
            returned(s, 4, EDGE)

    arrived_in(sec.at[:, :, pl.ds(0, 2 * EDGE)], send_sem.at[0])
    arrived_in(side.at[:, :, pl.ds(0, 2 * EDGE)], send_sem.at[1])
    arrived_in(other.at[:, :, pl.ds(1, block), pl.ds(0, 2 * EDGE)], send_sem.at[2])
    arrived_in(mixed, send_sem.at[3])
    arrived_in(pack_out, send_sem.at[4])
    arrived_in(mixed, send_sem.at[5])
    arrived_in(peaks_node, send_sem.at[6])
    arrived_in(peaks_space, send_sem.at[7])


def bands_of(rows):
    reach = SWEEPS - 1
    cut = rows - 4 * EDGE
    late = rows - 2 * EDGE
    lower = [(k - reach, cut + reach - k - EDGE) for k in range(SWEEPS)]
    middle = [(cut + reach - k - EDGE, late - k) for k in range(reach)] + [(cut - EDGE, cut + EDGE)]
    upper = [(late + EDGE + k, rows + reach - k) for k in range(reach)]
    last = [(late - k, late + EDGE + k) for k in range(reach)] + [(cut + EDGE, rows)]
    return lower, middle, upper, last


def finish(
    factors,
    swept,
    worst,
    side,
    in_a,
    in_b,
    in_c,
    in_d,
    in_e,
    out,
    residual,
    works_a,
    works_b,
    works_c,
    works_d,
    works_e,
    fresh,
    single,
    sem,
):
    works = (works_a, works_b, works_c, works_d, works_e)
    groups, cols = swept.shape[1:3]
    last = bands_of(groups * EDGE)[3]
    done = last[-1][0] // EDGE
    copies = [
        pltpu.make_async_copy(swept.at[0], out.at[0], sem.at[0]),
        pltpu.make_async_copy(swept.at[1, pl.ds(0, done)], out.at[1, pl.ds(0, done)], sem.at[1]),
        pltpu.make_async_copy(single, residual, sem.at[2]),
    ]
    copies[0].start()
    copies[1].start()
    single[...] = worst[pl.ds(0, 1), pl.ds(0, 1)]
    copies[2].start()
    me = lax.axis_index("node")
    factor = jnp.float32(factors[0])
    for m in range(1, len(factors)):
        factor = jnp.where(me == m, jnp.float32(factors[m]), factor)
    for k, (start, stop) in enumerate(last):
        for low in range(TOP + start, TOP + stop, EDGE):
            size = min(EDGE, TOP + stop - low)
            at = pl.ds(low, size)
            if k == 0:
                for c in range(cols):
                    works[0][0, c, at, :] = works[0][0, c, at, :] + side[1, c, at, :]
                continue
            sums = ringed_sums(works[k - 1], 0, low, size)
            for c in range(cols):
                value = side[1, c, at, :] + factor * sums[c]
                if k == SWEEPS - 1:
                    fresh[(low - TOP) // EDGE - done, c] = value
                else:
                    works[k][0, c, at, :] = value
            if k == SWEEPS - 1:
                g = (low - TOP) // EDGE
                copies.append(
                    pltpu.make_async_copy(fresh.at[g - done], out.at[1, g], sem.at[3 + g - done])
                )
                copies[-1].start()
    for copy in copies:
        copy.wait()


def shards(initial, sections, feed_rate, kill_rate):
    nodes = lax.axis_size("node")
    spaces = lax.axis_size("space")
    rows, columns = feed_rate.shape
    cols = columns // LANES
    block = cols // nodes
    doublings = (spaces - 1).bit_length()
    points, quad_matrix = radau_table(nodes)
    steps = step_size * np.float32(points)
    table = (
        step_size * np.float32(quad_matrix),
        steps,
        [1.0 / (4.0 * (steps * diff) + 1.0) for diff in (diff_u, diff_v)],
    )
    high = TOP + rows + TOP
    f32 = jnp.float32
    factors = steps * diff_v * table[2][1]

    def tiled(array):
        split = array.reshape(*array.shape[:-2], rows // EDGE, EDGE, cols, LANES)
        return jnp.swapaxes(split, -3, -2)

    any_spec = pl.BlockSpec(memory_space=pl.ANY)
    dma = pltpu.SemaphoreType.DMA
    vmem = pl.BlockSpec(memory_space=pltpu.VMEM)
    kept = (
        pltpu.VMEM((2, rows // EDGE, cols, EDGE, LANES), f32),
        pltpu.VMEM((EDGE, LANES), f32),
        pltpu.VMEM((2, cols, high, LANES), f32),
        *[pltpu.VMEM((1, cols, high, LANES), f32)] * (SWEEPS - 1),
    )
    room = 64 * 1024 * 1024 - 1024 * 1024 - sum(4 * int(np.prod(a.shape)) for a in kept)
    held = pl.pallas_call(
        functools.partial(kernel, nodes, spaces, table),
        out_shape=kept,
        in_specs=[any_spec] * 4,
        out_specs=(vmem,) * len(kept),
        scratch_shapes=[
            pltpu.VMEM((2, cols, high, LANES), f32),
            pltpu.VMEM((block, rows, LANES), f32),
            pltpu.VMEM((block, rows, LANES), f32),
            pltpu.VMEM((2, block, rows, LANES), f32),
            pltpu.VMEM((nodes - 1, 2, block + 2, high, LANES), f32),
            pltpu.VMEM((nodes - 1, 2, EDGE, LANES), f32),
            pltpu.VMEM((nodes - 1, 2, EDGE, LANES), f32),
            pltpu.VMEM((nodes - 1, 2, block, rows, LANES), f32),
            pltpu.VMEM((2 + doublings, EDGE, LANES), f32),
            pltpu.VMEM((nodes - 1, EDGE, LANES), f32),
            pltpu.VMEM((doublings, EDGE, LANES), f32),
            dma((4,)),
            dma((8,)),
            dma((3,)),
            dma((2, 4)),
            dma((2,)),
            dma((doublings,)),
            dma((4,)),
        ],
        compiler_params=pltpu.CompilerParams(
            collective_id=0, has_side_effects=True, vmem_limit_bytes=room
        ),
    )(*[tiled(a) for a in (sections[0], feed_rate, kill_rate, initial)])
    late = bands_of(rows)[3][-1]
    fresh = (late[1] - late[0]) // EDGE
    result, residual, *_ = pl.pallas_call(
        functools.partial(finish, factors),
        out_shape=(
            jax.ShapeDtypeStruct(kept[0].shape, f32),
            jax.ShapeDtypeStruct((1, 1), f32),
            *kept[3:],
        ),
        in_specs=[vmem] * len(kept),
        out_specs=(any_spec, any_spec, *[vmem] * (SWEEPS - 1)),
        scratch_shapes=[
            pltpu.VMEM((fresh, cols, EDGE, LANES), f32),
            pltpu.VMEM((1, 1), f32),
            dma((3 + fresh,)),
        ],
        input_output_aliases={3 + k: 2 + k for k in range(SWEEPS - 1)},
        compiler_params=pltpu.CompilerParams(vmem_limit_bytes=16 * 1024 * 1024),
    )(*held)
    result = jnp.swapaxes(result, -3, -2).reshape(sections.shape)
    return (result, residual.reshape(()))


def solution(mesh):
    placed = (
        P(None, "space", None),
        P("node", None, "space", None),
        P("space", None),
        P("space", None),
    )
    return jax.shard_map(
        shards,
        mesh=mesh,
        in_specs=placed,
        out_specs=(P("node", None, "space", None), P()),
        check_vma=False,
    )
```

```python
import functools

import jax
import jax.numpy as jnp
import numpy as np
from jax import lax
from jax.experimental import pallas as pl
from jax.experimental.pallas import tpu as pltpu
from jax.sharding import PartitionSpec as P

SWEEPS = 6


step_size = 4.0
diff_u = 1.0
diff_v = 0.5


def radau_target(order, value):
    before = 1.0
    current = value
    previous = 1.0
    for degree in range(1, order):
        following = ((2 * degree + 1) * value * current - degree * before) / (degree + 1)
        before = current
        current = following
    previous = before
    return current - previous


def radau_table(total):
    grid_count = 20000
    roots_found = []
    left_value = -1.0
    left_target = radau_target(total, left_value)
    for step_index in range(1, grid_count):
        right_value = -1.0 + 2.0 * step_index / grid_count
        right_target = radau_target(total, right_value)
        if left_target * right_target < 0.0:
            lower = left_value
            upper = right_value
            lower_target = left_target
            for bisect_index in range(80):
                halfway = 0.5 * (lower + upper)
                halfway_target = radau_target(total, halfway)
                if lower_target * halfway_target <= 0.0:
                    upper = halfway
                else:
                    lower = halfway
                    lower_target = halfway_target
            roots_found.append(0.5 * (lower + upper))
        left_value = right_value
        left_target = right_target
    roots_found.append(1.0)
    points = [(value + 1.0) / 2.0 for value in roots_found]
    quad_rows = []
    for node_index in range(total):
        row_values = []
        for basis_index in range(total):
            coefs = [1.0]
            for other_index in range(total):
                if other_index != basis_index:
                    scale = 1.0 / (points[basis_index] - points[other_index])
                    shifted = [0.0] + coefs
                    widened = coefs + [0.0]
                    coefs = [
                        (shifted[k] - points[other_index] * widened[k]) * scale
                        for k in range(len(shifted))
                    ]
            integral = 0.0
            for power_index in range(len(coefs)):
                integral += (
                    coefs[power_index] * points[node_index] ** (power_index + 1) / (power_index + 1)
                )
            row_values.append(integral)
        quad_rows.append(row_values)
    return (np.array(points), np.array(quad_rows))


MESH = pl.DeviceIdType.MESH
LANES = 128
EDGE = 8
TOP = 2 * EDGE


def ringed_sums(ref, s, start, size):
    cols = ref.shape[1]
    narrow = lax.broadcasted_iota(jnp.int32, (size, LANES), 1)
    at = pl.ds(start, size)
    tiles = [ref[s, k, at, :] for k in range(cols)]
    sums = []
    for k in range(cols):
        before, tile, after = tiles[k - 1], tiles[k], tiles[(k + 1) % cols]
        left = pltpu.roll(jnp.where(narrow == LANES - 1, before, tile), 1, 1)
        right = pltpu.roll(jnp.where(narrow == 0, after, tile), LANES - 1, 1)
        below = ref[s, k, pl.ds(start + 1, size), :]
        above = ref[s, k, pl.ds(start - 1, size), :]
        sums.append((below + above) + (right + left))
    return sums


def kernel(
    nodes,
    spaces,
    table,
    sections,
    feed_rate,
    kill_rate,
    initial,
    out,
    worst_out,
    side,
    works_a,
    works_b,
    works_c,
    works_d,
    works_e,
    sec,
    feed,
    kill,
    init,
    other,
    pack_out,
    pack_in,
    mixed,
    peak,
    peaks_node,
    peaks_space,
    local_sem,
    send_sem,
    first_sem,
    second_sem,
    side_sem,
    peak_sem,
    misc_sem,
):
    works = (works_a, works_b, works_c, works_d, works_e)
    cols = sec.shape[1]
    rows = feed.shape[1]
    block = cols // nodes
    me = lax.axis_index("node")
    here = lax.axis_index("space")
    tall = 2 if nodes % 2 == 0 else 1
    wide = nodes // tall
    chunks = (
        (0, TOP),
        (rows - TOP, TOP),
        (TOP, rows - 5 * EDGE),
        (rows - 3 * EDGE, EDGE),
    )
    pieces = (
        (0, EDGE),
        (rows - EDGE, EDGE),
        (EDGE, rows - 5 * EDGE),
        (rows - 4 * EDGE, 2 * EDGE),
        (rows - 2 * EDGE, EDGE),
    )
    own = me * block

    def moved(m, o):
        return ((m // wide + o // wide) % tall) * wide + (m % wide + o % wide) % wide

    def ahead(o):
        return moved(me, o)

    def negated(o):
        return ((tall - o // wide) % tall) * wide + (wide - o % wide) % wide

    def fetch(source, target, start, size, offset, sem):
        for k in range(start // EDGE, (start + size) // EDGE):
            pltpu.make_async_copy(
                source.at[k], target.at[:, pl.ds(offset + k * EDGE, EDGE)], sem
            ).start()

    def arrived_in(ref, sem):
        pltpu.make_async_copy(ref, ref, sem).wait()

    barrier = pltpu.get_barrier_semaphore()
    for o in range(1, nodes):
        pl.semaphore_signal(barrier, inc=1, device_id={"node": ahead(o)}, device_id_type=MESH)
    for o in (1, spaces - 1):
        pl.semaphore_signal(
            barrier, inc=1, device_id={"space": (here + o) % spaces}, device_id_type=MESH
        )

    for i, (start, size) in enumerate(chunks):
        for s in range(2):
            fetch(sections.at[s], sec.at[s], start, size, TOP, local_sem.at[i // 2])

    mine = pl.ds(own, block)
    fetch(feed_rate.at[:, mine], feed, 0, rows, 0, local_sem.at[2])
    fetch(kill_rate.at[:, mine], kill, 0, rows, 0, local_sem.at[2])
    for s in range(2):
        fetch(initial.at[s, :, mine], init.at[s], 0, rows, 0, local_sem.at[3])

    def along(ref, sent, received, way):
        start = TOP + rows - EDGE if way == 0 else TOP
        land = TOP - EDGE if way == 0 else TOP + rows
        target = (here + 1) % spaces if way == 0 else (here + spaces - 1) % spaces
        return pltpu.make_async_remote_copy(
            src_ref=ref.at[:, pl.ds(start, EDGE)],
            dst_ref=ref.at[:, pl.ds(land, EDGE)],
            send_sem=sent,
            recv_sem=received,
            device_id={"space": target},
            device_id_type=MESH,
        )

    def sec_halo(s, way):
        return along(sec.at[s], send_sem.at[0], misc_sem.at[0], way)

    def side_halo(s, way):
        return along(side.at[s], send_sem.at[1], side_sem.at[s], way)

    def forward(o, s, way):
        return along(
            other.at[o - 1, s, pl.ds(1, block)], send_sem.at[2], misc_sem.at[1], way
        )

    def first(p, o):
        start, size = chunks[p]
        where = pl.ds(TOP + start, size)
        return pltpu.make_async_remote_copy(
            src_ref=sec.at[:, pl.ds(ahead(o) * block, block), where],
            dst_ref=other.at[o - 1, :, pl.ds(1, block), where],
            send_sem=send_sem.at[3],
            recv_sem=first_sem.at[max(p - 1, 0)],
            device_id={"node": ahead(o)},
            device_id_type=MESH,
        )

    def packed(o):
        return pltpu.make_async_remote_copy(
            src_ref=pack_out.at[o - 1],
            dst_ref=pack_in.at[o - 1],
            send_sem=send_sem.at[4],
            recv_sem=misc_sem.at[2],
            device_id={"node": ahead(o)},
            device_id_type=MESH,
        )

    def second(s, p, o):
        start, size = pieces[p]
        return pltpu.make_async_remote_copy(
            src_ref=mixed.at[o - 1, s, :, pl.ds(start, size)],
            dst_ref=side.at[s, mine, pl.ds(TOP + start, size)],
            send_sem=send_sem.at[5],
            recv_sem=second_sem.at[s, max(p - 1, 0)],
            device_id={"node": ahead(o)},
            device_id_type=MESH,
        )

    order = tuple(range(nodes - 1, 0, -1))
    lane = lax.broadcasted_iota(jnp.int32, (EDGE, LANES), 1)

    arrived_in(sec.at[:, :, pl.ds(TOP, 2 * TOP)], local_sem.at[0])
    pl.semaphore_wait(barrier, nodes - 1 + 2)
    for p in range(2):
        for o in order:
            first(p, o).start()
    for s in range(2):
        for way in range(2):
            sec_halo(s, way).start()
    arrived_in(sec.at[:, :, pl.ds(TOP, rows - 2 * TOP)], local_sem.at[1])

    groups = rows // EDGE
    for o in order:
        left = (ahead(o) * block + cols - 1) % cols
        right = (ahead(o) * block + block) % cols
        for s in range(2):
            pack = jnp.zeros((EDGE, LANES), jnp.float32)
            for g in range(groups):
                at = pl.ds(TOP + g * EDGE, EDGE)
                both = jnp.where(lane == LANES - 1, sec[s, left, at, :], sec[s, right, at, :])
                pack = jnp.where(lane // 2 == g, pltpu.roll(both, 2 * g + 1, 1), pack)
            pack_out[o - 1, s] = pack
        packed(o).start()
    for p in range(2, 4):
        for o in order:
            first(p, o).start()

    arrived_in(init, local_sem.at[2])
    arrived_in(init, local_sem.at[3])

    def first_arrived(p, size):
        arrived_in(other.at[:, :, pl.ds(1, block), pl.ds(TOP, size)], first_sem.at[p])

    first_arrived(0, 2 * TOP)
    for o in order:
        for s in range(2):
            for way in range(2):
                forward(o, s, way).start()
    arrived_in(pack_in, misc_sem.at[2])
    for o in order:
        for s in range(2):
            pack = pack_in[o - 1, s]
            for g in range(groups):
                at = pl.ds(TOP + g * EDGE, EDGE)
                both = pltpu.roll(pack, LANES - 1 - 2 * g, 1)
                other[o - 1, s, 0, at, :] = both
                other[o - 1, s, block + 1, at, :] = both
    arrived_in(sec.at[:, :, pl.ds(0, 2 * EDGE)], misc_sem.at[0])
    arrived_in(other.at[:, :, pl.ds(1, block), pl.ds(0, 2 * EDGE)], misc_sem.at[1])

    diffs = (diff_u, diff_v)

    def chosen(entries):
        value = jnp.float32(entries[0])
        for m in range(1, nodes):
            value = jnp.where(me == m, jnp.float32(entries[m]), value)
        return value

    every = range(nodes)
    quads, step_table, inverse_table = table
    weights = [
        [chosen([quads[moved(m, t), moved(m, negated(j))] for m in every]) for j in every]
        for t in every
    ]
    steps = [chosen([step_table[moved(m, t)] for m in every]) for t in every]
    inverses = [[chosen([inverse_table[s][moved(m, t)] for m in every]) for t in every] for s in range(2)]

    def ringed(left, middle, right, start):
        at = pl.ds(TOP + start, EDGE)
        here_tile = middle[at, :]
        before = pltpu.roll(jnp.where(lane == LANES - 1, left[at, :], here_tile), 1, 1)
        after = pltpu.roll(jnp.where(lane == 0, right[at, :], here_tile), LANES - 1, 1)
        below = middle[pl.ds(TOP + start + 1, EDGE), :]
        above = middle[pl.ds(TOP + start - 1, EDGE), :]
        return here_tile, (below + above) + (after + before)

    def mix(starts, worst):
        def one(c, worst):
            here_column = own + c
            left = (own + c + cols - 1) % cols
            right = (own + c + 1) % cols
            for start in starts:
                at = pl.ds(start, EDGE)
                f = feed[c, at, :]
                both_rates = f + kill[c, at, :]
                fields, laps, slopes = ([], []), ([], []), ([], [])
                for slot in range(nodes):
                    for s in range(2):
                        if slot == 0:
                            tiles = [sec.at[s, k] for k in (left, here_column, right)]
                        else:
                            tiles = [other.at[slot - 1, s, c + k] for k in range(3)]
                        w, ring = ringed(*tiles, start)
                        fields[s].append(w)
                        laps[s].append(diffs[s] * (ring - 4.0 * w))
                    u, v = fields[0][slot], fields[1][slot]
                    product = u * v * v
                    slopes[0].append(laps[0][slot] + (f * (1.0 - u) - product))
                    slopes[1].append(laps[1][slot] + (product - both_rates * v))
                for s in range(2):
                    base = init[s, c, at, :]
                    for t in range(nodes):
                        to = negated(t)
                        total = weights[t][0] * slopes[s][0]
                        for j in range(1, nodes):
                            total = total + weights[t][j] * slopes[s][j]
                        total = base + total
                        worst = jnp.maximum(worst, jnp.abs(total - fields[s][to]))
                        value = (total - steps[t] * laps[s][to]) * inverses[s][t]
                        if t == 0:
                            side[s, here_column, pl.ds(TOP + start, EDGE), :] = value
                        else:
                            mixed[t - 1, s, c, at, :] = value
            return worst

        return lax.fori_loop(0, block, one, worst)

    def edges(p, o):
        start, size = pieces[p]
        return pltpu.make_async_remote_copy(
            src_ref=mixed.at[o - 1, :, :, pl.ds(start, size)],
            dst_ref=side.at[:, mine, pl.ds(TOP + start, size)],
            send_sem=send_sem.at[5],
            recv_sem=second_sem.at[0, 0],
            device_id={"node": ahead(o)},
            device_id_type=MESH,
        )

    def send_back(s, ps):
        for p in ps:
            for o in order:
                second(s, p, o).start()

    def starts_of(ps):
        return [low for p in ps for low in range(pieces[p][0], sum(pieces[p]), EDGE)]

    worst = jnp.zeros((EDGE, LANES), jnp.float32)
    worst = mix(starts_of((0, 1)), worst)
    for p in range(2):
        for o in order:
            edges(p, o).start()
    first_arrived(1, chunks[2][1])
    worst = mix(starts_of((2,)), worst)
    send_back(0, (2,))
    first_arrived(2, chunks[3][1])
    worst = mix(starts_of((3, 4)), worst)
    peak[0] = worst

    def peak_node(o):
        return pltpu.make_async_remote_copy(
            src_ref=peak.at[0],
            dst_ref=peaks_node.at[o - 1],
            send_sem=send_sem.at[6],
            recv_sem=misc_sem.at[3],
            device_id={"node": ahead(o)},
            device_id_type=MESH,
        )

    def peak_space(k):
        apart = 2**k
        return pltpu.make_async_remote_copy(
            src_ref=peak.at[1 + k],
            dst_ref=peaks_space.at[k],
            send_sem=send_sem.at[7],
            recv_sem=peak_sem.at[k],
            device_id={"space": here + apart - here // apart % 2 * 2 * apart},
            device_id_type=MESH,
        )

    doublings = peaks_space.shape[0]
    peak_steps = list(range(doublings))
    pace = -(-doublings // 3)

    def peak_advance():
        for k in peak_steps[:pace]:
            arrived_in(peaks_space.at[k], peak_sem.at[k])
            peak[2 + k] = jnp.maximum(peak[1 + k], peaks_space[k])
            if k + 1 < doublings:
                peak_space(k + 1).start()
        del peak_steps[:pace]

    for o in range(1, nodes):
        peak_node(o).start()
    send_back(0, (3, 4))
    send_back(1, (2, 3, 4))

    inverse = [inverses[s][0] for s in range(2)]
    factor = [steps[0] * diffs[s] * inverse[s] for s in range(2)]

    def put(s, k, low, size, values):
        for c in range(cols):
            if k == SWEEPS - 1:
                out[s, (low - TOP) // EDGE, c] = values[c]
            else:
                works[k][0, c, pl.ds(low, size), :] = values[c]

    def steps_in(span):
        start, stop = span
        return [(low, min(EDGE, TOP + stop - low)) for low in range(TOP + start, TOP + stop, EDGE)]

    def band(s, spans):
        for k, span in enumerate(spans):
            source, plane = (sec, s) if k == 0 else (works[k - 1], 0)
            for low, size in steps_in(span):
                sums = ringed_sums(source, plane, low, size)
                put(s, k, low, size, [
                    side[s, c, pl.ds(low, size), :] + factor[s] * sums[c] for c in range(cols)
                ])

    lower, middle, upper, last = bands_of(rows)

    def returned(s, p, size):
        arrived_in(mixed.at[:, s, :, pl.ds(0, size)], second_sem.at[s, p - 1])

    arrived_in(mixed.at[:, :, :, pl.ds(0, 2 * EDGE)], second_sem.at[0, 0])
    for s in range(2):
        for way in range(2):
            side_halo(s, way).start()

    for s in range(2):
        arrived_in(side.at[s, :, pl.ds(0, 2 * EDGE)], side_sem.at[s])
        band(s, upper)
        if s == 1:
            peak_advance()
        returned(s, 2, pieces[2][1])
        band(s, lower)
        if s == 0:
            arrived_in(peaks_node, misc_sem.at[3])
            peak[1] = jnp.maximum(peak[0], jnp.max(peaks_node[...], axis=0))
            peak_space(0).start()
        else:
            peak_advance()
            worst_out[...] = jnp.full((EDGE, LANES), jnp.max(peak[1 + doublings]))
        returned(s, 3, pieces[3][1])
        band(s, middle)
        if s == 0:
            peak_advance()
            returned(s, 4, EDGE)
            band(s, last)
        else:
            for low, size in steps_in(last[0]):
                sums = ringed_sums(sec, s, low, size)
                put(s, 0, low, size, [factor[s] * total for total in sums])
            returned(s, 4, EDGE)

    arrived_in(sec.at[:, :, pl.ds(0, 2 * EDGE)], send_sem.at[0])
    arrived_in(side.at[:, :, pl.ds(0, 2 * EDGE)], send_sem.at[1])
    arrived_in(other.at[:, :, pl.ds(1, block), pl.ds(0, 2 * EDGE)], send_sem.at[2])
    arrived_in(mixed, send_sem.at[3])
    arrived_in(pack_out, send_sem.at[4])
    arrived_in(mixed, send_sem.at[5])
    arrived_in(peaks_node, send_sem.at[6])
    arrived_in(peaks_space, send_sem.at[7])


def bands_of(rows):
    reach = SWEEPS - 1
    cut = rows - 4 * EDGE
    late = rows - 2 * EDGE
    lower = [(k - reach, cut + reach - k - EDGE) for k in range(SWEEPS)]
    middle = [(cut + reach - k - EDGE, late - k) for k in range(reach)] + [(cut - EDGE, cut + EDGE)]
    upper = [(late + EDGE + k, rows + reach - k) for k in range(reach)]
    last = [(late - k, late + EDGE + k) for k in range(reach)] + [(cut + EDGE, rows)]
    return lower, middle, upper, last


def finish(
    factors,
    swept,
    worst,
    side,
    in_a,
    in_b,
    in_c,
    in_d,
    in_e,
    out,
    residual,
    works_a,
    works_b,
    works_c,
    works_d,
    works_e,
    fresh,
    single,
    sem,
):
    works = (works_a, works_b, works_c, works_d, works_e)
    groups, cols = swept.shape[1:3]
    last = bands_of(groups * EDGE)[3]
    done = last[-1][0] // EDGE
    copies = [
        pltpu.make_async_copy(swept.at[0], out.at[0], sem.at[0]),
        pltpu.make_async_copy(swept.at[1, pl.ds(0, done)], out.at[1, pl.ds(0, done)], sem.at[1]),
        pltpu.make_async_copy(single, residual, sem.at[2]),
    ]
    copies[0].start()
    copies[1].start()
    single[...] = worst[pl.ds(0, 1), pl.ds(0, 1)]
    copies[2].start()
    me = lax.axis_index("node")
    factor = jnp.float32(factors[0])
    for m in range(1, len(factors)):
        factor = jnp.where(me == m, jnp.float32(factors[m]), factor)
    for k, (start, stop) in enumerate(last):
        for low in range(TOP + start, TOP + stop, EDGE):
            size = min(EDGE, TOP + stop - low)
            at = pl.ds(low, size)
            if k == 0:
                for c in range(cols):
                    works[0][0, c, at, :] = works[0][0, c, at, :] + side[1, c, at, :]
                continue
            sums = ringed_sums(works[k - 1], 0, low, size)
            for c in range(cols):
                value = side[1, c, at, :] + factor * sums[c]
                if k == SWEEPS - 1:
                    fresh[(low - TOP) // EDGE - done, c] = value
                else:
                    works[k][0, c, at, :] = value
            if k == SWEEPS - 1:
                g = (low - TOP) // EDGE
                copies.append(
                    pltpu.make_async_copy(fresh.at[g - done], out.at[1, g], sem.at[3 + g - done])
                )
                copies[-1].start()
    for copy in copies:
        copy.wait()


def shards(initial, sections, feed_rate, kill_rate):
    nodes = lax.axis_size("node")
    spaces = lax.axis_size("space")
    rows, columns = feed_rate.shape
    cols = columns // LANES
    block = cols // nodes
    doublings = (spaces - 1).bit_length()
    points, quad_matrix = radau_table(nodes)
    steps = step_size * np.float32(points)
    table = (
        step_size * np.float32(quad_matrix),
        steps,
        [1.0 / (4.0 * (steps * diff) + 1.0) for diff in (diff_u, diff_v)],
    )
    high = TOP + rows + TOP
    f32 = jnp.float32
    factors = steps * diff_v * table[2][1]

    def tiled(array):
        split = array.reshape(*array.shape[:-2], rows // EDGE, EDGE, cols, LANES)
        return jnp.swapaxes(split, -3, -2)

    any_spec = pl.BlockSpec(memory_space=pl.ANY)
    dma = pltpu.SemaphoreType.DMA
    vmem = pl.BlockSpec(memory_space=pltpu.VMEM)
    kept = (
        pltpu.VMEM((2, rows // EDGE, cols, EDGE, LANES), f32),
        pltpu.VMEM((EDGE, LANES), f32),
        pltpu.VMEM((2, cols, high, LANES), f32),
        *[pltpu.VMEM((1, cols, high, LANES), f32)] * (SWEEPS - 1),
    )
    room = 64 * 1024 * 1024 - 1024 * 1024 - sum(4 * int(np.prod(a.shape)) for a in kept)
    held = pl.pallas_call(
        functools.partial(kernel, nodes, spaces, table),
        out_shape=kept,
        in_specs=[any_spec] * 4,
        out_specs=(vmem,) * len(kept),
        scratch_shapes=[
            pltpu.VMEM((2, cols, high, LANES), f32),
            pltpu.VMEM((block, rows, LANES), f32),
            pltpu.VMEM((block, rows, LANES), f32),
            pltpu.VMEM((2, block, rows, LANES), f32),
            pltpu.VMEM((nodes - 1, 2, block + 2, high, LANES), f32),
            pltpu.VMEM((nodes - 1, 2, EDGE, LANES), f32),
            pltpu.VMEM((nodes - 1, 2, EDGE, LANES), f32),
            pltpu.VMEM((nodes - 1, 2, block, rows, LANES), f32),
            pltpu.VMEM((2 + doublings, EDGE, LANES), f32),
            pltpu.VMEM((nodes - 1, EDGE, LANES), f32),
            pltpu.VMEM((doublings, EDGE, LANES), f32),
            dma((4,)),
            dma((8,)),
            dma((3,)),
            dma((2, 4)),
            dma((2,)),
            dma((doublings,)),
            dma((4,)),
        ],
        compiler_params=pltpu.CompilerParams(
            collective_id=0, has_side_effects=True, vmem_limit_bytes=room
        ),
    )(*[tiled(a) for a in (sections[0], feed_rate, kill_rate, initial)])
    late = bands_of(rows)[3][-1]
    fresh = (late[1] - late[0]) // EDGE
    result, residual, *_ = pl.pallas_call(
        functools.partial(finish, factors),
        out_shape=(
            jax.ShapeDtypeStruct(kept[0].shape, f32),
            jax.ShapeDtypeStruct((1, 1), f32),
            *kept[3:],
        ),
        in_specs=[vmem] * len(kept),
        out_specs=(any_spec, any_spec, *[vmem] * (SWEEPS - 1)),
        scratch_shapes=[
            pltpu.VMEM((fresh, cols, EDGE, LANES), f32),
            pltpu.VMEM((1, 1), f32),
            dma((3 + fresh,)),
        ],
        input_output_aliases={3 + k: 2 + k for k in range(SWEEPS - 1)},
        compiler_params=pltpu.CompilerParams(vmem_limit_bytes=16 * 1024 * 1024),
    )(*held)
    result = jnp.swapaxes(result, -3, -2).reshape(sections.shape)
    return (result, residual.reshape(()))


def solution(mesh):
    placed = (
        P(None, "space", None),
        P("node", None, "space", None),
        P("space", None),
        P("space", None),
    )
    return jax.shard_map(
        shards,
        mesh=mesh,
        in_specs=placed,
        out_specs=(P("node", None, "space", None), P()),
        check_vma=False,
    )
```
